32 devices in a mesh: grp: 4 (over z), dev: 8 (over y, x, core).
Axes of the slice: x: 2, y: 2, z: 4, core: 2. Of those that a mesh axis runs over, the one named last changes fastest.
Arguments:
- amounts: float32 [64, 524288], P('dev', 'grp'), may hold values from -0.06 to 0.06, as said below
Outputs:
- offsets: float32 [64, 524288], P(None, ('grp', 'dev'))
The draws below stay inside these ranges and needn't reach their ends.
Inputs may be any that keep to these rules, and one draw needn't show every extreme that they name: `amounts`: each entry lies within 0.06 of zero.
All inputs are finite; a program needn't handle non-finite values.
Results may differ from the reference program's by a relative error of at most 0.00095.
Values sent between devices are 32-bit elements; how exact they have to be, the bound alone decides.
A program may use at most 64 MiB of HBM per device.

```python
import jax
import jax.numpy as jnp

COLS = 64
ROW_DEV = 16384
ROWS = 524288


def draw_amounts(key, part):
    subkeys = jax.random.split(jax.random.fold_in(key, 17), 3)
    regions = ROWS // (ROW_DEV // 4)
    noise = jax.random.uniform(subkeys[0], (COLS, ROWS + 1), jnp.float32, -1.0, 1.0)
    reach = 1.0
    drift = jax.random.uniform(subkeys[2], (COLS, 1), jnp.float32, 0.0, 2.0)
    factor = jnp.exp(jax.random.uniform(subkeys[1], (COLS, regions), jnp.float32, -reach, reach))
    factor = jnp.repeat(factor, ROW_DEV // 4, axis=1, total_repeat_length=ROWS)
    rough = 0.01 * (noise[:, 1:] - noise[:, :-1])
    values = factor * (rough + drift / ROWS)
    return values.astype(jnp.float32)


def setup_inputs(seed: int = 0) -> dict:
    arg_keys = jax.random.split(jax.random.key(seed), 2)
    amounts = draw_amounts(jax.random.fold_in(arg_keys[1], 71), 0)
    return {"amounts": amounts}


def exclusive_rows(values, block_len):
    chans, length = values.shape
    blocks = values.reshape(chans, length // block_len, block_len)
    within = jnp.cumsum(blocks, axis=2) - blocks
    sums = jnp.sum(blocks, axis=2)
    starts = jnp.cumsum(sums, axis=1) - sums
    return (within + starts[:, :, None]).reshape(chans, length)


def reference(amounts):
    return exclusive_rows(amounts, 512)
```

```python
import functools

import jax
import jax.numpy as jnp
from jax import lax
from jax.experimental import pallas as pl
from jax.experimental.pallas import tpu as pltpu
from jax.sharding import PartitionSpec as P

MESH = pl.DeviceIdType.MESH
LANES = 128
VMEM_GRANT = 46 << 20


def flip(me, k):
    other, bit = me, 1
    while bit <= k:
        if k & bit:
            other = other + bit - 2 * bit * lax.rem(me // bit, 2)
        bit *= 2
    return other


def classes(n):
    across = (1 << (n.bit_length() - 2) // 2) - 1 << 1
    down = n - 2 - across
    order = sorted(range(2, n), key=lambda k: (k & 1, k))
    xs = [k for k in order if not k & down]
    ys = [k for k in order if not k & across]
    ds = [k for k in order if k & across and k & down]
    return across, xs, ys, ds


def tile_of(rows):
    return min(rows // 8, 2048)


def scan_tile(block, w_ref, run):
    chans, tile = block.shape
    steps = tile // LANES
    stack = jnp.concatenate([block[:, j * LANES:(j + 1) * LANES] for j in range(steps)], axis=0)
    high = stack.astype(jnp.bfloat16)
    rest = stack - high.astype(jnp.float32)
    mid = rest.astype(jnp.bfloat16)
    low = (rest - mid.astype(jnp.float32)).astype(jnp.bfloat16)
    sums = jnp.dot(jnp.concatenate([high, mid], axis=1), w_ref[...], preferred_element_type=jnp.float32)
    sums = sums + jnp.dot(low, w_ref[:LANES, :], preferred_element_type=jnp.float32)
    parts = []
    for j in range(steps):
        part = sums[j * chans:(j + 1) * chans]
        parts.append(part[:, :LANES] + run)
        run = run + part[:, LANES:]
    return parts, run


def exchange(n, groups, x_ref, t_ref, run_ref, w_ref, x_vm, relay_vm, give_vm, carry_vm, group_vm,
             load_sem, send_sem, recv_sem, hsend_sem, hrecv_sem, csend_sem, crecv_sem, zsend_sem, zrecv_sem,
             note_sem, ready_sem, zready_sem):
    me, grp = lax.axis_index("dev"), lax.axis_index("grp")
    core = lax.rem(me, 2)
    base = me - core
    chans, rows = t_ref.shape[1:]
    tile = tile_of(rows)
    across, xs, ys, ds = classes(n)
    late = (xs[-1], ds[-1])
    others = {k: flip(me, k) for k in range(n)}
    x_chips = [k for k in xs if not k & 1]
    y_chips = [k for k in ys if not k & 1]

    def signal(sem, **device):
        pl.semaphore_signal(sem, inc=1, device_id=device, device_id_type=MESH)

    barrier = pltpu.get_barrier_semaphore()
    for k in y_chips:
        signal(barrier, dev=flip(base, k) + 1)
    for k in x_chips:
        signal(barrier, dev=flip(base, k))

    @pl.when(core == 1)
    def _():
        signal(barrier, dev=base)

    @pl.when(grp > 0)
    def _():
        signal(barrier, grp=grp - 1, dev=0)

    def part(k, lo, size):
        return pl.ds(pl.multiple_of(others[k] * rows + lo, LANES), size)

    def load(k):
        return pltpu.make_async_copy(x_ref.at[:, part(k, 0, rows)], x_vm.at[:, part(k, 0, rows)], load_sem.at[k])

    for pair in zip(ys, ds):
        for k in pair:
            load(k).start()
    for k in [*ys[len(ds):], *ds[len(ys):], *xs, 1, 0]:
        load(k).start()

    def spans(k):
        cuts = [0, rows // 2, rows - tile, rows] if k in late else [0, rows]
        return list(enumerate(zip(cuts[:-1], cuts[1:])))

    def direct(k, piece, lo, hi, source):
        return pltpu.make_async_remote_copy(
            src_ref=x_vm.at[:, part(k, lo, hi - lo)], dst_ref=t_ref.at[source, :, pl.ds(lo, hi - lo)],
            send_sem=send_sem.at[piece, others[k]], recv_sem=recv_sem.at[piece, source],
            device_id={"dev": others[k]}, device_id_type=MESH)

    def hop(k):
        slot = ds.index(k)
        return pltpu.make_async_remote_copy(
            src_ref=x_vm.at[:, part(k, 0, rows)], dst_ref=relay_vm.at[slot],
            send_sem=hsend_sem.at[slot], recv_sem=hrecv_sem.at[slot],
            device_id={"dev": others[k & across]}, device_id_type=MESH)

    def relay(k, piece, lo, hi, source):
        slot = ds.index(k)
        return pltpu.make_async_remote_copy(
            src_ref=relay_vm.at[slot, :, pl.ds(lo, hi - lo)], dst_ref=t_ref.at[source, :, pl.ds(lo, hi - lo)],
            send_sem=send_sem.at[piece, others[k]], recv_sem=recv_sem.at[piece, source],
            device_id={"dev": others[k & ~across]}, device_id_type=MESH)

    def send(ks):
        for k in ks:
            load(k).wait()
            for piece, (lo, hi) in spans(k):
                direct(k, piece, lo, hi, me).start()

    def send_hops():
        for k in ds:
            load(k).wait()
            hop(k).start()

    @pl.when(core == 0)
    def _():
        after = jnp.where((me == 0) & (grp < groups - 1), n, 0)
        pl.semaphore_wait(barrier, 1 + 2 * len(x_chips) + after)
        signal(note_sem, dev=base + 1)
        send_hops()
        pl.semaphore_wait(note_sem, 1)
        send(ys)

    @pl.when(core == 1)
    def _():
        pl.semaphore_wait(barrier, 2 * len(y_chips))
        send(ys)
        pl.semaphore_wait(note_sem, 1)
        signal(note_sem, dev=base)
        for k in x_chips:
            signal(ready_sem, dev=flip(base, k))
            signal(ready_sem, dev=flip(base, k) + 1)
        send_hops()

    send([1])
    for k in [*xs, 0]:
        load(k).wait()

    shape = (2 * LANES, 2 * LANES)
    row = lax.rem(lax.broadcasted_iota(jnp.int32, shape, 0), LANES)
    col = lax.broadcasted_iota(jnp.int32, shape, 1)
    w_ref[...] = jnp.where((row < col) | (col >= LANES), 1.0, 0.0).astype(jnp.bfloat16)

    def range_total(j, total):
        give_vm[j] = total

        def one(i, acc):
            block = x_vm[:, pl.ds(pl.multiple_of(j * rows + i * tile, LANES), tile)]
            parts = [block[:, s * LANES:(s + 1) * LANES] for s in range(tile // LANES)]
            while len(parts) > 1:
                parts = [a + b for a, b in zip(parts[::2], parts[1::2])] + parts[len(parts) & ~1:]
            return acc + parts[0]

        acc = lax.fori_loop(0, rows // tile, one, jnp.zeros((chans, LANES), jnp.float32))
        return total + jnp.broadcast_to(jnp.sum(acc, axis=1, keepdims=True), acc.shape)

    total = lax.fori_loop(0, n, range_total, jnp.zeros((chans, LANES), jnp.float32))

    pl.semaphore_wait(ready_sem, len(x_chips))

    @pl.when((me == 0) & (grp < groups - 1))
    def _():
        for k in range(1, n):
            signal(zready_sem, dev=k)

    def pass_on():
        return pltpu.make_async_remote_copy(
            src_ref=group_vm.at[1], dst_ref=group_vm.at[0], send_sem=zsend_sem, recv_sem=zrecv_sem,
            device_id={"grp": grp + 1}, device_id_type=MESH)

    @pl.when((me > 0) & (grp < groups - 1))
    def _():
        pl.semaphore_wait(zready_sem, 1)

    @pl.when(grp == 0)
    def _():
        group_vm[0] = jnp.zeros_like(total)

    @pl.when(grp > 0)
    def _():
        pass_on().wait_recv()

    before = group_vm[0]
    group_vm[1] = before + total
    for j in range(n):
        give_vm[j] = give_vm[j] + before
    carry_vm[me] = give_vm[me]

    @pl.when(grp < groups - 1)
    def _():
        pass_on().start()

    def give(k, source):
        return pltpu.make_async_remote_copy(
            src_ref=give_vm.at[others[k]], dst_ref=carry_vm.at[source],
            send_sem=csend_sem.at[others[k]], recv_sem=crecv_sem.at[source],
            device_id={"dev": others[k]}, device_id_type=MESH)

    for k in [1, *ys, *xs, *ds]:
        give(k, me).start()
    for k in xs:
        for piece, (lo, hi) in spans(k):
            direct(k, piece, lo, hi, me).start()

    def scan(source, start, dest, lo, hi, run):
        def one(i, run):
            parts, run = scan_tile(source[:, pl.ds(pl.multiple_of(start + lo + i * tile, LANES), tile)], w_ref, run)
            for j, sums in enumerate(parts):
                dest[:, pl.ds(pl.multiple_of(lo + i * tile + j * LANES, LANES), LANES)] = sums
            return run

        return lax.fori_loop(0, (hi - lo) // tile, one, run)

    scan(x_vm, me * rows, t_ref.at[me], 0, rows, carry_vm[me])

    def arrived(k, piece, lo, hi):
        copy = relay if k in ds else direct
        copy(k, piece, lo, hi, others[k]).wait_recv()

    def finish(k):
        give(k, others[k]).wait_recv()
        arrived(k, 0, 0, rows)
        block = t_ref.at[others[k]]
        scan(block, 0, block, 0, rows, carry_vm[others[k]])

    finish(1)
    for k in ds:
        hop(k).wait_recv()
        for piece, (lo, hi) in spans(k):
            relay(k, piece, lo, hi, others[k & across]).start()
    for k in ys:
        finish(k)
    rest = [k for pair in zip(xs, ds) for k in pair] + xs[len(ds):] + ds[len(xs):]
    for k in rest:
        if k not in late:
            finish(k)
    runs = {}
    for k in late:
        give(k, others[k]).wait_recv()
        runs[k] = carry_vm[others[k]]
    *early, last = spans(late[0])
    for piece, (lo, hi) in early:
        for k in late:
            arrived(k, piece, lo, hi)
            block = t_ref.at[others[k]]
            runs[k] = scan(block, 0, block, lo, hi, runs[k])
    for i, k in enumerate(late):
        run_ref[i] = runs[k]

    @pl.when(grp < groups - 1)
    def _():
        pass_on().wait_send()

    for k in range(1, n):
        give(k, me).wait_send()
    for k in ds:
        hop(k).wait_send()
    for k in range(1, n):
        for piece, (lo, hi) in spans(k):
            (relay if k in ds else direct)(k, piece, lo, hi, me).wait_send()
    for k in late:
        arrived(k, last[0], *last[1])


def write(n, t_ref, run_ref, w_ref, out_ref, stage, main_sem, last_sem):
    me = lax.axis_index("dev")
    rows = t_ref.shape[2]
    tile = tile_of(rows)
    _, xs, _, ds = classes(n)
    late = (xs[-1], ds[-1])
    main, last = pl.ds(0, rows - tile), pl.ds(rows - tile, tile)

    def whole(k):
        at = flip(me, k)
        if k in late:
            return pltpu.make_async_copy(t_ref.at[at, :, main], out_ref.at[at, :, main], main_sem.at[k])
        return pltpu.make_async_copy(t_ref.at[at], out_ref.at[at], main_sem.at[k])

    def tail(i, k):
        return pltpu.make_async_copy(stage.at[i], out_ref.at[flip(me, k), :, last], last_sem.at[i])

    for k in range(n):
        whole(k).start()
    for i, k in enumerate(late):
        parts, _ = scan_tile(t_ref[flip(me, k), :, last], w_ref, run_ref[i])
        for j, sums in enumerate(parts):
            stage[i, :, pl.ds(j * LANES, LANES)] = sums
        tail(i, k).start()
    for k in range(n):
        whole(k).wait()
    for i, k in enumerate(late):
        tail(i, k).wait()


def solution(mesh):
    n, groups = mesh.shape["dev"], mesh.shape["grp"]
    assert n >= 8 and not n & (n - 1)

    def local(amounts):
        chans, length = amounts.shape
        rows = length // n
        tile = tile_of(rows)
        diagonals = len(classes(n)[3])
        f32 = jnp.float32
        dma = pltpu.SemaphoreType.DMA
        regular = pltpu.SemaphoreType.REGULAR
        wide = (2 * LANES, 2 * LANES)
        table, run, weights = pl.pallas_call(
            functools.partial(exchange, n, groups),
            out_shape=[jax.ShapeDtypeStruct((n, chans, rows), f32),
                       jax.ShapeDtypeStruct((2, chans, LANES), f32),
                       jax.ShapeDtypeStruct(wide, jnp.bfloat16)],
            in_specs=[pl.BlockSpec(memory_space=pl.ANY)],
            out_specs=[pl.BlockSpec(memory_space=pltpu.VMEM)] * 3,
            scratch_shapes=[
                pltpu.VMEM((chans, length), f32),
                pltpu.VMEM((diagonals, chans, rows), f32),
                pltpu.VMEM((n, chans, LANES), f32),
                pltpu.VMEM((n, chans, LANES), f32),
                pltpu.VMEM((2, chans, LANES), f32),
                dma((n,)), dma((3, n)), dma((3, n)), dma((diagonals,)), dma((diagonals,)),
                dma((n,)), dma((n,)), dma, dma, regular, regular, regular,
            ],
            compiler_params=pltpu.CompilerParams(
                collective_id=0, has_side_effects=True, vmem_limit_bytes=VMEM_GRANT),
            name="exchange",
        )(amounts)
        out = pl.pallas_call(
            functools.partial(write, n),
            out_shape=jax.ShapeDtypeStruct((n, chans, rows), f32),
            in_specs=[pl.BlockSpec(memory_space=pltpu.VMEM)] * 3,
            out_specs=pl.BlockSpec(memory_space=pl.ANY),
            scratch_shapes=[pltpu.VMEM((2, chans, tile), f32), dma((n,)), dma((2,))],
            compiler_params=pltpu.CompilerParams(vmem_limit_bytes=VMEM_GRANT),
            name="write",
        )(table, run, weights)
        return out.reshape(n * chans, rows)

    return jax.shard_map(
        local,
        mesh=mesh,
        in_specs=(P("dev", "grp"),),
        out_specs=P(None, ("grp", "dev")),
        check_vma=False,
    )
```

```python
import functools

import jax
import jax.numpy as jnp
from jax import lax
from jax.experimental import pallas as pl
from jax.experimental.pallas import tpu as pltpu
from jax.sharding import PartitionSpec as P

MESH = pl.DeviceIdType.MESH
LANES = 128
VMEM_GRANT = 46 << 20


def flip(me, k):
    other, bit = me, 1
    while bit <= k:
        if k & bit:
            other = other + bit - 2 * bit * lax.rem(me // bit, 2)
        bit *= 2
    return other


def chips(n):
    across = (1 << (n.bit_length() - 2) // 2) - 1 << 1
    flips = range(2, n, 2)
    xs = [k for k in flips if not k & ~across]
    ys = [k for k in flips if not k & across]
    ds = [k for k in flips if k & across and k & ~across]
    return across, xs, ys, ds


def late_flips(n):
    _, xs, _, ds = chips(n)
    return [k + core for k in [*xs, *ds] for core in (0, 1)]


def tile_of(rows):
    return min(rows // 8, 2048)


def cuts_of(rows):
    cuts = [0, rows // 4, rows // 2, 3 * rows // 4, rows - tile_of(rows), rows]
    return list(zip(cuts[:-1], cuts[1:]))


def scan_tiles(blocks, w_ref, runs):
    chans, width = blocks[0].shape
    steps = width // LANES
    stack = jnp.concatenate(
        [block[:, j * LANES:(j + 1) * LANES] for block in blocks for j in range(steps)], axis=0)
    high = stack.astype(jnp.bfloat16)
    rest = stack - high.astype(jnp.float32)
    mid = rest.astype(jnp.bfloat16)
    low = (rest - mid.astype(jnp.float32)).astype(jnp.bfloat16)
    sums = jnp.dot(jnp.concatenate([high, mid], axis=1), w_ref[...], preferred_element_type=jnp.float32)
    sums = sums + jnp.dot(low, w_ref[:LANES, :], preferred_element_type=jnp.float32)
    outs, after = [], []
    for i, run in enumerate(runs):
        parts = []
        for j in range(i * steps, (i + 1) * steps):
            part = sums[j * chans:(j + 1) * chans]
            parts.append(part[:, :LANES] + run)
            run = run + part[:, LANES:]
        outs.append(parts)
        after.append(run)
    return outs, after


def exchange(n, groups, x_ref, t_ref, run_ref, w_ref, x_vm, relay_vm, give_vm, carry_vm, group_vm,
             load_sem, send_sem, recv_sem, hsend_sem, hrecv_sem, csend_sem, crecv_sem, zsend_sem, zrecv_sem,
             note_sem, ready_sem, hello_sem, zready_sem):
    me, grp = lax.axis_index("dev"), lax.axis_index("grp")
    core = lax.rem(me, 2)
    base = me - core
    partner = base + 1 - core
    chans, rows = t_ref.shape[1:]
    tile = tile_of(rows)
    pieces = cuts_of(rows)
    whole = [(0, rows)]
    across, xs, ys, ds = chips(n)
    late = [flip(me, k) for k in late_flips(n)]

    def x_core(chip):
        return jnp.where(lax.rem(chip // 2, across // 2 + 1) > 0, 1, 0)

    def targets(k):
        chip = flip(base, k)
        first = jnp.where((chip == 0) & (grp == 0), 0, 1)
        return [chip + first, chip + 1 - first]

    def signal(sem, **device):
        pl.semaphore_signal(sem, inc=1, device_id=device, device_id_type=MESH)

    barrier = pltpu.get_barrier_semaphore()
    for k in ys:
        signal(barrier, dev=flip(base, k) + 1 - x_core(base))
    for k in xs:
        signal(barrier, dev=flip(base, k) + x_core(flip(base, k)))

    @pl.when(core == 1)
    def _():
        signal(barrier, dev=base)

    @pl.when((me == 0) & (grp > 0))
    def _():
        signal(barrier, grp=grp - 1, dev=0)

    def at(j, lo=0, size=rows):
        return pl.ds(pl.multiple_of(j * rows + lo, LANES), size)

    def load(sem, j, lo=0, size=rows):
        return pltpu.make_async_copy(x_ref.at[:, at(j, lo, size)], x_vm.at[:, at(j, lo, size)], load_sem.at[sem])

    def remote(src, dst, sems, device):
        return pltpu.make_async_remote_copy(
            src_ref=src, dst_ref=dst, send_sem=sems[0], recv_sem=sems[1],
            device_id=device, device_id_type=MESH)

    def direct(j, sem, lo, hi):
        remote(x_vm.at[:, at(j, lo, hi - lo)], t_ref.at[me, :, pl.ds(lo, hi - lo)],
               (send_sem, recv_sem.at[sem]), {"dev": j}).start()

    def hop(j, slot, lo, hi):
        remote(x_vm.at[:, at(j, lo, hi - lo)], relay_vm.at[slot, :, pl.ds(lo, hi - lo)],
               (hsend_sem, hrecv_sem.at[slot]), {"dev": flip(me, ds[slot // 2] & across)}).start()

    def relay(j, slot, sem, lo, hi):
        source = flip(me, ds[slot // 2] & across)
        remote(relay_vm.at[slot, :, pl.ds(lo, hi - lo)], t_ref.at[source, :, pl.ds(lo, hi - lo)],
               (send_sem, recv_sem.at[sem]), {"dev": j}).start()

    x_blocks = [j for k in xs for j in targets(k)]
    y_blocks = [j for k in ys for j in targets(k)]
    d_blocks = [j for k in ds for j in targets(k)]

    def send_y(slots, spans):
        for slot in slots:
            for lo, hi in spans:
                direct(y_blocks[slot], 1, lo, hi)

    def send_d(slots, spans):
        for slot in slots:
            for lo, hi in spans:
                hop(d_blocks[slot], slot, lo, hi)

    turns = [(core == x_core(base), d_blocks, y_blocks, send_d, send_y),
             (core != x_core(base), y_blocks, d_blocks, send_y, send_d)]

    for mine, first, second, _, _ in turns:
        @pl.when(mine)
        def _():
            load(0, first[0], 0, tile).start()
            load(1, first[0], tile, rows - tile).start()
            for j in [*first[1:], *second]:
                load(2, j).start()

    for j in [*x_blocks, me, partner]:
        load(2, j).start()

    after = jnp.where((me == 0) & (grp < groups - 1), 1, 0)
    faced = jnp.where(core == x_core(base), 2 * len(xs), 2 * len(ys))
    pl.semaphore_wait(barrier, faced + 1 - core + after)

    for mine, first, _, send_first, _ in turns:
        @pl.when(mine)
        def _():
            load(0, first[0], 0, tile).wait()
            send_first([0], [(0, tile)])
            load(1, first[0], tile, rows - tile).wait()
            send_first([0], [(tile, rows)])

    @pl.when(core == 0)
    def _():
        signal(note_sem, dev=base + 1)

    @pl.when((me == 0) & (grp < groups - 1))
    def _():
        signal(hello_sem, grp=grp + 1)

    @pl.when(core == 1)
    def _():
        pl.semaphore_wait(note_sem, 1)
        signal(note_sem, dev=base)
        for k in xs:
            signal(ready_sem, dev=flip(base, k))
            signal(ready_sem, dev=flip(base, k) + 1)

    load(2, 0, 0, (n - 1) * rows).wait()
    for mine, first, _, send_first, _ in turns:
        @pl.when(mine)
        def _():
            send_first(range(1, len(first)), whole)

    @pl.when(core == 0)
    def _():
        pl.semaphore_wait(note_sem, 1)

    for mine, _, second, _, send_second in turns:
        @pl.when(mine)
        def _():
            send_second(range(len(second)), whole)

    direct(partner, 0, 0, rows)

    shape = (2 * LANES, 2 * LANES)
    row = lax.rem(lax.broadcasted_iota(jnp.int32, shape, 0), LANES)
    col = lax.broadcasted_iota(jnp.int32, shape, 1)
    w_ref[...] = jnp.where((row < col) | (col >= LANES), 1.0, 0.0).astype(jnp.bfloat16)

    def range_total(j, total):
        give_vm[j] = total

        def one(i, acc):
            block = x_vm[:, at(j, i * tile, tile)]
            parts = [block[:, s * LANES:(s + 1) * LANES] for s in range(tile // LANES)]
            while len(parts) > 1:
                parts = [a + b for a, b in zip(parts[::2], parts[1::2])] + parts[len(parts) & ~1:]
            return acc + parts[0]

        acc = lax.fori_loop(0, rows // tile, one, jnp.zeros((chans, LANES), jnp.float32))
        return total + jnp.broadcast_to(jnp.sum(acc, axis=1, keepdims=True), acc.shape)

    total = lax.fori_loop(0, n, range_total, jnp.zeros((chans, LANES), jnp.float32))

    pl.semaphore_wait(ready_sem, len(xs))

    @pl.when((me == 0) & (grp > 0))
    def _():
        pl.semaphore_wait(hello_sem, 1)
        signal(zready_sem, grp=grp - 1)

    @pl.when(grp < groups - 1)
    def _():
        pl.semaphore_wait(zready_sem, 1)

    @pl.when((me == 0) & (grp < groups - 1))
    def _():
        for k in range(1, n):
            signal(zready_sem, dev=k)

    def pass_on():
        return remote(group_vm.at[1], group_vm.at[0], (zsend_sem, zrecv_sem), {"grp": grp + 1})

    @pl.when(grp == 0)
    def _():
        group_vm[0] = jnp.zeros_like(total)

    @pl.when(grp > 0)
    def _():
        pass_on().wait_recv()

    before = group_vm[0]
    group_vm[1] = before + total
    for j in range(n):
        give_vm[j] = give_vm[j] + before
    carry_vm[me] = give_vm[me]

    @pl.when(grp < groups - 1)
    def _():
        pass_on().start()

    for j in [partner, *y_blocks, *x_blocks, *d_blocks]:
        remote(give_vm.at[j], carry_vm.at[me], (csend_sem, crecv_sem), {"dev": j}).start()
    for j in x_blocks:
        for i, (lo, hi) in enumerate(pieces):
            direct(j, 2 + i, lo, hi)

    def scan(blocks, lo, hi, runs):
        width = min(hi - lo, 4 * tile // len(blocks))

        def one(i, runs):
            start = lo + i * width
            tiles = [source[:, pl.ds(pl.multiple_of(offset + start, LANES), width)] for source, offset, _ in blocks]
            outs, runs = scan_tiles(tiles, w_ref, runs)
            for (_, _, dest), parts in zip(blocks, outs):
                for j, sums in enumerate(parts):
                    dest[:, pl.ds(pl.multiple_of(start + j * LANES, LANES), LANES)] = sums
            return tuple(runs)

        return lax.fori_loop(0, (hi - lo) // width, one, tuple(runs))

    def in_place(j):
        return t_ref.at[j], 0, t_ref.at[j]

    def arrived(sem, blocks, lo=0, hi=rows):
        span = t_ref.at[pl.ds(0, blocks), :, pl.ds(lo, hi - lo)]
        remote(span, span, (send_sem, recv_sem.at[sem]), {"dev": partner}).wait_recv()

    scan([(x_vm, me * rows, t_ref.at[me])], 0, rows, [carry_vm[me]])
    for slot in range(len(d_blocks)):
        remote(relay_vm.at[slot], relay_vm.at[slot], (hsend_sem, hrecv_sem.at[slot]), {"dev": partner}).wait_recv()
        j = targets(ds[slot // 2] & ~across)[slot % 2]
        for i, (lo, hi) in enumerate(pieces):
            relay(j, slot, 2 + i, lo, hi)

    gives = carry_vm.at[pl.ds(0, n - 1)]
    remote(gives, gives, (csend_sem, crecv_sem), {"dev": partner}).wait()
    arrived(0, 1)
    scan([in_place(partner)], 0, rows, [carry_vm[partner]])
    arrived(1, len(y_blocks))
    for s in range(0, len(y_blocks), 2):
        pair = y_blocks[s:s + 2]
        scan([in_place(j) for j in pair], 0, rows, [carry_vm[j] for j in pair])

    for i, j in enumerate(late):
        run_ref[i] = carry_vm[j]
    for i, (lo, hi) in enumerate(pieces[:-1]):
        arrived(2 + i, len(late), lo, hi)
        for s in range(0, len(late), 4):
            four = late[s:s + 4]
            runs = scan([in_place(j) for j in four], lo, hi, [run_ref[s + r] for r in range(len(four))])
            for r, run in enumerate(runs):
                run_ref[s + r] = run

    @pl.when(grp < groups - 1)
    def _():
        pass_on().wait_send()

    remote(relay_vm, relay_vm, (hsend_sem, hrecv_sem.at[0]), {"dev": partner}).wait_send()
    sent = x_vm.at[:, pl.ds(0, (n - 1) * rows)]
    remote(sent, sent, (send_sem, recv_sem.at[0]), {"dev": partner}).wait_send()
    arrived(1 + len(pieces), len(late), *pieces[-1])


def write(n, t_ref, run_ref, w_ref, out_ref, stage, sem):
    me = lax.axis_index("dev")
    rows = t_ref.shape[2]
    tile = tile_of(rows)
    late = late_flips(n)
    main, last = pl.ds(0, rows - tile), pl.ds(rows - tile, tile)

    for k in range(n):
        j = flip(me, k)
        if k in late:
            pltpu.make_async_copy(t_ref.at[j, :, main], out_ref.at[j, :, main], sem).start()
        else:
            pltpu.make_async_copy(t_ref.at[j], out_ref.at[j], sem).start()
    for s in range(0, len(late), 4):
        four = late[s:s + 4]
        outs, _ = scan_tiles([t_ref[flip(me, k), :, last] for k in four], w_ref, [run_ref[s + r] for r in range(len(four))])
        for r, (k, parts) in enumerate(zip(four, outs)):
            for j, sums in enumerate(parts):
                stage[s + r, :, pl.ds(j * LANES, LANES)] = sums
            pltpu.make_async_copy(stage.at[s + r], out_ref.at[flip(me, k), :, last], sem).start()
    pltpu.make_async_copy(t_ref, out_ref, sem).wait()


def solution(mesh):
    n, groups = mesh.shape["dev"], mesh.shape["grp"]
    assert n >= 8 and not n & (n - 1)

    def local(amounts):
        chans, length = amounts.shape
        rows = length // n
        tile = tile_of(rows)
        late = len(late_flips(n))
        relays = 2 * len(chips(n)[3])
        f32 = jnp.float32
        dma = pltpu.SemaphoreType.DMA
        regular = pltpu.SemaphoreType.REGULAR
        wide = (2 * LANES, 2 * LANES)
        table, run, weights = pl.pallas_call(
            functools.partial(exchange, n, groups),
            out_shape=[jax.ShapeDtypeStruct((n, chans, rows), f32),
                       jax.ShapeDtypeStruct((late, chans, LANES), f32),
                       jax.ShapeDtypeStruct(wide, jnp.bfloat16)],
            in_specs=[pl.BlockSpec(memory_space=pl.ANY)],
            out_specs=[pl.BlockSpec(memory_space=pltpu.VMEM)] * 3,
            scratch_shapes=[
                pltpu.VMEM((chans, length), f32),
                pltpu.VMEM((relays, chans, rows), f32),
                pltpu.VMEM((n, chans, LANES), f32),
                pltpu.VMEM((n, chans, LANES), f32),
                pltpu.VMEM((2, chans, LANES), f32),
                dma((3,)), dma, dma((2 + len(cuts_of(rows)),)), dma, dma((relays,)),
                dma, dma, dma, dma, regular, regular, regular, regular,
            ],
            compiler_params=pltpu.CompilerParams(
                collective_id=0, has_side_effects=True, vmem_limit_bytes=VMEM_GRANT),
            name="exchange",
        )(amounts)
        out = pl.pallas_call(
            functools.partial(write, n),
            out_shape=jax.ShapeDtypeStruct((n, chans, rows), f32),
            in_specs=[pl.BlockSpec(memory_space=pltpu.VMEM)] * 3,
            out_specs=pl.BlockSpec(memory_space=pl.ANY),
            scratch_shapes=[pltpu.VMEM((late, chans, tile), f32), dma],
            compiler_params=pltpu.CompilerParams(vmem_limit_bytes=VMEM_GRANT),
            name="write",
        )(table, run, weights)
        return out.reshape(n * chans, rows)

    return jax.shard_map(
        local,
        mesh=mesh,
        in_specs=(P("dev", "grp"),),
        out_specs=P(None, ("grp", "dev")),
        check_vma=False,
    )
```

```python
import functools

import jax
import jax.numpy as jnp
from jax import lax
from jax.experimental import pallas as pl
from jax.experimental.pallas import tpu as pltpu
from jax.sharding import PartitionSpec as P

MESH = pl.DeviceIdType.MESH
LANES = 128
VMEM_GRANT = 46 << 20


def flip(me, k):
    other, bit = me, 1
    while bit <= k:
        if k & bit:
            other = other + bit - 2 * bit * lax.rem(me // bit, 2)
        bit *= 2
    return other


def chips(n):
    across = (1 << (n.bit_length() - 2) // 2) - 1 << 1
    flips = range(2, n, 2)
    xs = [k for k in flips if not k & ~across]
    ys = [k for k in flips if not k & across]
    ds = [k for k in flips if k & across and k & ~across]
    return across, xs, ys, ds


def late_flips(n):
    _, xs, _, ds = chips(n)
    return [k + core for k in [*xs, *ds] for core in (0, 1)]


def tile_of(rows):
    return min(rows // 8, 2048)


def cuts_of(rows):
    cuts = [0, rows // 2, 3 * rows // 4, rows - tile_of(rows), rows]
    return list(zip(cuts[:-1], cuts[1:]))


def scan_tiles(blocks, w_ref, runs):
    chans, width = blocks[0].shape
    steps = width // LANES
    stack = jnp.concatenate(
        [block[:, j * LANES:(j + 1) * LANES] for block in blocks for j in range(steps)], axis=0)
    high = stack.astype(jnp.bfloat16)
    rest = stack - high.astype(jnp.float32)
    mid = rest.astype(jnp.bfloat16)
    low = (rest - mid.astype(jnp.float32)).astype(jnp.bfloat16)
    sums = jnp.dot(jnp.concatenate([high, mid], axis=1), w_ref[...], preferred_element_type=jnp.float32)
    sums = sums + jnp.dot(low, w_ref[:LANES, :], preferred_element_type=jnp.float32)
    outs, after = [], []
    for i, run in enumerate(runs):
        parts = []
        for j in range(i * steps, (i + 1) * steps):
            part = sums[j * chans:(j + 1) * chans]
            parts.append(part[:, :LANES] + run)
            run = run + part[:, LANES:]
        outs.append(parts)
        after.append(run)
    return outs, after


def exchange(n, groups, x_ref, t_ref, run_ref, w_ref, x_vm, relay_vm, give_vm, carry_vm, group_vm,
             load_sem, send_sem, recv_sem, hsend_sem, hrecv_sem, csend_sem, crecv_sem, zsend_sem, zrecv_sem,
             note_sem, ready_sem, far_sem, hello_sem, zready_sem):
    me, grp = lax.axis_index("dev"), lax.axis_index("grp")
    core = lax.rem(me, 2)
    base = me - core
    partner = base + 1 - core
    chans, rows = t_ref.shape[1:]
    tile = tile_of(rows)
    pieces = cuts_of(rows)
    whole = [(0, rows)]
    across, xs, ys, ds = chips(n)
    late = [flip(me, k) for k in late_flips(n)]

    def x_core(chip):
        return jnp.where((chip > across) & (lax.rem(chip // 2, across // 2 + 1) == 0), 0, 1)

    def y_core(chip):
        return jnp.where((chip <= across) & (chip > 0), 0, 1)

    def lead(chip):
        return jnp.where((chip == 0) & (grp == 0), 0, 1)

    def targets(k):
        chip = flip(base, k)
        return [chip + lead(chip), chip + 1 - lead(chip)]

    def signal(sem, **device):
        pl.semaphore_signal(sem, inc=1, device_id=device, device_id_type=MESH)

    barrier = pltpu.get_barrier_semaphore()

    @pl.when(core == lead(base))
    def _():
        for k in ys:
            signal(barrier, dev=flip(base, k) + y_core(flip(base, k)))
        for k in xs:
            signal(barrier, dev=flip(base, k) + x_core(flip(base, k)))

    @pl.when(core == 1)
    def _():
        signal(barrier, dev=base)

    @pl.when((me == 1) & (grp > 0))
    def _():
        signal(barrier, grp=grp - 1)

    def at(j, lo=0, size=rows):
        return pl.ds(pl.multiple_of(j * rows + lo, LANES), size)

    def load(sem, j, lo=0, size=rows):
        return pltpu.make_async_copy(x_ref.at[:, at(j, lo, size)], x_vm.at[:, at(j, lo, size)], load_sem.at[sem])

    def remote(src, dst, sems, device):
        return pltpu.make_async_remote_copy(
            src_ref=src, dst_ref=dst, send_sem=sems[0], recv_sem=sems[1],
            device_id=device, device_id_type=MESH)

    def direct(j, sem, lo, hi):
        remote(x_vm.at[:, at(j, lo, hi - lo)], t_ref.at[me, :, pl.ds(lo, hi - lo)],
               (send_sem, recv_sem.at[sem]), {"dev": j}).start()

    def hop(j, slot, lo, hi):
        remote(x_vm.at[:, at(j, lo, hi - lo)], relay_vm.at[slot, :, pl.ds(lo, hi - lo)],
               (hsend_sem, hrecv_sem.at[slot]), {"dev": flip(me, ds[slot // 2] & across)}).start()

    def relay(j, slot, sem, lo, hi):
        source = flip(me, ds[slot // 2] & across)
        remote(relay_vm.at[slot, :, pl.ds(lo, hi - lo)], t_ref.at[source, :, pl.ds(lo, hi - lo)],
               (send_sem, recv_sem.at[sem]), {"dev": j}).start()

    x_blocks = [j for k in xs for j in targets(k)]
    y_blocks = [j for k in ys for j in targets(k)]
    d_blocks = [j for k in ds for j in targets(k)]

    def send_y(slots, spans):
        for slot in slots:
            for lo, hi in spans:
                direct(y_blocks[slot], 0, lo, hi)

    def send_d():
        for slot, j in enumerate(d_blocks):
            hop(j, slot, 0, rows)

    half = rows // 2
    x_side, y_side = core == x_core(base), core == y_core(base)
    openings = [(0, x_blocks[0], 0, tile), (1, y_blocks[0], 0, tile),
                (2, x_blocks[0], tile, half), (3, y_blocks[0], tile, rows)]
    for sem, j, lo, hi in openings:
        load(sem, j, lo, hi - lo).start()
    for j in [*d_blocks, *y_blocks[1:], *x_blocks[1:], me, partner]:
        load(4, j).start()
    load(4, x_blocks[0], half, half).start()

    def await_opening(i):
        sem, j, lo, hi = openings[i]
        load(sem, j, lo, hi - lo).wait()

    after = jnp.where((me == 1) & (grp < groups - 1), 1, 0)
    faced = jnp.where(x_side, len(xs), 0) + jnp.where(y_side, len(ys), 0)
    pl.semaphore_wait(barrier, faced + 1 - core + after)

    for i in range(4):
        await_opening(i)

        @pl.when(y_side if i % 2 else x_side)
        def _():
            _, j, lo, hi = openings[i]
            direct(j, 0 if i % 2 else 1, lo, hi)

    @pl.when(core == 0)
    def _():
        signal(note_sem, dev=base + 1)

    @pl.when((me == 1) & (grp < groups - 1))
    def _():
        signal(hello_sem, grp=grp + 1)

    pl.semaphore_wait(note_sem, 1)

    @pl.when(core == 1)
    def _():
        signal(note_sem, dev=base)
        for k in [*xs, *ys]:
            signal(ready_sem, dev=targets(k)[0])

    pl.semaphore_wait(ready_sem, jnp.where(core == lead(base), len(xs) + len(ys), 1))

    @pl.when(core == lead(base))
    def _():
        signal(ready_sem, dev=partner)

    @pl.when(core == 1)
    def _():
        for k in xs:
            for j in targets(k):
                signal(far_sem, dev=j)

    load(4, 0, 0, (n - 2) * rows + half).wait()
    send_d()

    @pl.when(jnp.logical_not(y_side))
    def _():
        send_y([0], whole)

    send_y(range(1, len(y_blocks)), whole)
    direct(partner, 0, 0, rows)

    shape = (2 * LANES, 2 * LANES)
    row = lax.rem(lax.broadcasted_iota(jnp.int32, shape, 0), LANES)
    col = lax.broadcasted_iota(jnp.int32, shape, 1)
    w_ref[...] = jnp.where((row < col) | (col >= LANES), 1.0, 0.0).astype(jnp.bfloat16)

    def range_total(j, total):
        give_vm[j] = total

        def one(i, acc):
            block = x_vm[:, at(j, i * tile, tile)]
            parts = [block[:, s * LANES:(s + 1) * LANES] for s in range(tile // LANES)]
            while len(parts) > 1:
                parts = [a + b for a, b in zip(parts[::2], parts[1::2])] + parts[len(parts) & ~1:]
            return acc + parts[0]

        acc = lax.fori_loop(0, rows // tile, one, jnp.zeros((chans, LANES), jnp.float32))
        return total + jnp.broadcast_to(jnp.sum(acc, axis=1, keepdims=True), acc.shape)

    total = lax.fori_loop(0, n, range_total, jnp.zeros((chans, LANES), jnp.float32))

    pl.semaphore_wait(far_sem, len(xs))

    @pl.when((me == 1) & (grp > 0))
    def _():
        pl.semaphore_wait(hello_sem, 1)
        signal(zready_sem, grp=grp - 1)

    @pl.when(grp < groups - 1)
    def _():
        pl.semaphore_wait(zready_sem, 1)

    @pl.when((me == 1) & (grp < groups - 1))
    def _():
        for k in range(1, n):
            signal(zready_sem, dev=flip(me, k))

    def pass_on():
        return remote(group_vm.at[1], group_vm.at[0], (zsend_sem, zrecv_sem), {"grp": grp + 1})

    @pl.when(grp == 0)
    def _():
        group_vm[0] = jnp.zeros_like(total)

    @pl.when(grp > 0)
    def _():
        pass_on().wait_recv()

    before = group_vm[0]
    group_vm[1] = before + total
    for j in range(n):
        give_vm[j] = give_vm[j] + before
    carry_vm[me] = give_vm[me]

    @pl.when(grp < groups - 1)
    def _():
        pass_on().start()

    for j in [partner, *y_blocks, *x_blocks, *d_blocks]:
        remote(give_vm.at[j], carry_vm.at[me], (csend_sem, crecv_sem), {"dev": j}).start()

    @pl.when(jnp.logical_not(x_side))
    def _():
        direct(x_blocks[0], 1, 0, half)

    for slot, j in enumerate(x_blocks):
        for i, (lo, hi) in enumerate(pieces):
            if slot or i:
                direct(j, 1 + i, lo, hi)

    def scan(blocks, lo, hi, runs):
        width = min(hi - lo, 4 * tile // len(blocks))

        def one(i, runs):
            start = lo + i * width
            tiles = [source[:, pl.ds(pl.multiple_of(offset + start, LANES), width)] for source, offset, _ in blocks]
            outs, runs = scan_tiles(tiles, w_ref, runs)
            for (_, _, dest), parts in zip(blocks, outs):
                for j, sums in enumerate(parts):
                    dest[:, pl.ds(pl.multiple_of(start + j * LANES, LANES), LANES)] = sums
            return tuple(runs)

        return lax.fori_loop(0, (hi - lo) // width, one, tuple(runs))

    def in_place(j):
        return t_ref.at[j], 0, t_ref.at[j]

    def arrived(sem, blocks, lo=0, hi=rows):
        span = t_ref.at[pl.ds(0, blocks), :, pl.ds(lo, hi - lo)]
        remote(span, span, (send_sem, recv_sem.at[sem]), {"dev": partner}).wait_recv()

    scan([(x_vm, me * rows, t_ref.at[me])], 0, rows, [carry_vm[me]])
    for slot in range(len(d_blocks)):
        remote(relay_vm.at[slot], relay_vm.at[slot], (hsend_sem, hrecv_sem.at[slot]), {"dev": partner}).wait_recv()
        j = targets(ds[slot // 2] & ~across)[slot % 2]
        for i, (lo, hi) in enumerate(pieces):
            relay(j, slot, 1 + i, lo, hi)

    gives = carry_vm.at[pl.ds(0, n - 1)]
    remote(gives, gives, (csend_sem, crecv_sem), {"dev": partner}).wait()
    arrived(0, 1 + len(y_blocks))
    scan([in_place(partner)], 0, rows, [carry_vm[partner]])
    for s in range(0, len(y_blocks), 2):
        pair = y_blocks[s:s + 2]
        scan([in_place(j) for j in pair], 0, rows, [carry_vm[j] for j in pair])

    for i, j in enumerate(late):
        run_ref[i] = carry_vm[j]
    for i, (lo, hi) in enumerate(pieces[:-1]):
        arrived(1 + i, len(late), lo, hi)
        for s in range(0, len(late), 4):
            four = late[s:s + 4]
            runs = scan([in_place(j) for j in four], lo, hi, [run_ref[s + r] for r in range(len(four))])
            for r, run in enumerate(runs):
                run_ref[s + r] = run

    @pl.when(grp < groups - 1)
    def _():
        pass_on().wait_send()

    remote(relay_vm, relay_vm, (hsend_sem, hrecv_sem.at[0]), {"dev": partner}).wait_send()
    sent = x_vm.at[:, pl.ds(0, (n - 1) * rows)]
    remote(sent, sent, (send_sem, recv_sem.at[0]), {"dev": partner}).wait_send()
    arrived(len(pieces), len(late), *pieces[-1])


def write(n, t_ref, run_ref, w_ref, out_ref, stage, sem):
    me = lax.axis_index("dev")
    rows = t_ref.shape[2]
    tile = tile_of(rows)
    late = late_flips(n)
    main, last = pl.ds(0, rows - tile), pl.ds(rows - tile, tile)

    for k in range(n):
        j = flip(me, k)
        if k in late:
            pltpu.make_async_copy(t_ref.at[j, :, main], out_ref.at[j, :, main], sem).start()
        else:
            pltpu.make_async_copy(t_ref.at[j], out_ref.at[j], sem).start()
    for s in range(0, len(late), 4):
        four = late[s:s + 4]
        outs, _ = scan_tiles([t_ref[flip(me, k), :, last] for k in four], w_ref, [run_ref[s + r] for r in range(len(four))])
        for r, (k, parts) in enumerate(zip(four, outs)):
            for j, sums in enumerate(parts):
                stage[s + r, :, pl.ds(j * LANES, LANES)] = sums
            pltpu.make_async_copy(stage.at[s + r], out_ref.at[flip(me, k), :, last], sem).start()
    pltpu.make_async_copy(t_ref, out_ref, sem).wait()


def solution(mesh):
    n, groups = mesh.shape["dev"], mesh.shape["grp"]
    assert n >= 8 and not n & (n - 1)

    def local(amounts):
        chans, length = amounts.shape
        rows = length // n
        tile = tile_of(rows)
        late = len(late_flips(n))
        relays = 2 * len(chips(n)[3])
        f32 = jnp.float32
        dma = pltpu.SemaphoreType.DMA
        regular = pltpu.SemaphoreType.REGULAR
        wide = (2 * LANES, 2 * LANES)
        table, run, weights = pl.pallas_call(
            functools.partial(exchange, n, groups),
            out_shape=[jax.ShapeDtypeStruct((n, chans, rows), f32),
                       jax.ShapeDtypeStruct((late, chans, LANES), f32),
                       jax.ShapeDtypeStruct(wide, jnp.bfloat16)],
            in_specs=[pl.BlockSpec(memory_space=pl.ANY)],
            out_specs=[pl.BlockSpec(memory_space=pltpu.VMEM)] * 3,
            scratch_shapes=[
                pltpu.VMEM((chans, length), f32),
                pltpu.VMEM((relays, chans, rows), f32),
                pltpu.VMEM((n, chans, LANES), f32),
                pltpu.VMEM((n, chans, LANES), f32),
                pltpu.VMEM((2, chans, LANES), f32),
                dma((5,)), dma, dma((1 + len(cuts_of(rows)),)), dma, dma((relays,)),
                dma, dma, dma, dma, regular, regular, regular, regular, regular,
            ],
            compiler_params=pltpu.CompilerParams(
                collective_id=0, has_side_effects=True, vmem_limit_bytes=VMEM_GRANT),
            name="exchange",
        )(amounts)
        out = pl.pallas_call(
            functools.partial(write, n),
            out_shape=jax.ShapeDtypeStruct((n, chans, rows), f32),
            in_specs=[pl.BlockSpec(memory_space=pltpu.VMEM)] * 3,
            out_specs=pl.BlockSpec(memory_space=pl.ANY),
            scratch_shapes=[pltpu.VMEM((late, chans, tile), f32), dma],
            compiler_params=pltpu.CompilerParams(vmem_limit_bytes=VMEM_GRANT),
            name="write",
        )(table, run, weights)
        return out.reshape(n * chans, rows)

    return jax.shard_map(
        local,
        mesh=mesh,
        in_specs=(P("dev", "grp"),),
        out_specs=P(None, ("grp", "dev")),
        check_vma=False,
    )
```

```python
import functools

import jax
import jax.numpy as jnp
from jax import lax
from jax.experimental import pallas as pl
from jax.experimental.pallas import tpu as pltpu
from jax.sharding import PartitionSpec as P

MESH = pl.DeviceIdType.MESH
LANES = 128
VMEM_GRANT = 46 << 20


def flip(me, k):
    other, bit = me, 1
    while bit <= k:
        if k & bit:
            other = other + bit - 2 * bit * lax.rem(me // bit, 2)
        bit *= 2
    return other


def chips(n):
    across = (1 << (n.bit_length() - 2) // 2) - 1 << 1
    flips = range(2, n, 2)
    xs = [k for k in flips if not k & ~across]
    ys = [k for k in flips if not k & across]
    ds = [k for k in flips if k & across and k & ~across]
    return across, xs, ys, ds


def late_flips(n):
    _, xs, _, ds = chips(n)
    return [k + core for k in [*xs, *ds] for core in (0, 1)]


def tile_of(rows):
    return min(rows // 8, 2048)


def cuts_of(rows):
    cuts = [0, rows // 2, 3 * rows // 4, rows - tile_of(rows), rows]
    return list(zip(cuts[:-1], cuts[1:]))


def scan_tiles(blocks, w_ref, runs):
    chans, width = blocks[0].shape
    steps = width // LANES
    stack = jnp.concatenate(
        [block[:, j * LANES:(j + 1) * LANES] for block in blocks for j in range(steps)], axis=0)
    high = stack.astype(jnp.bfloat16)
    rest = stack - high.astype(jnp.float32)
    mid = rest.astype(jnp.bfloat16)
    low = (rest - mid.astype(jnp.float32)).astype(jnp.bfloat16)
    sums = jnp.dot(jnp.concatenate([high, mid], axis=1), w_ref[...], preferred_element_type=jnp.float32)
    sums = sums + jnp.dot(low, w_ref[:LANES, :], preferred_element_type=jnp.float32)
    outs, after = [], []
    for i, run in enumerate(runs):
        parts = []
        for j in range(i * steps, (i + 1) * steps):
            part = sums[j * chans:(j + 1) * chans]
            parts.append(part[:, :LANES] + run)
            run = run + part[:, LANES:]
        outs.append(parts)
        after.append(run)
    return outs, after


def exchange(n, groups, x_ref, t_ref, run_ref, w_ref, x_vm, relay_vm, give_vm, carry_vm, group_vm,
             load_sem, send_sem, recv_sem, hsend_sem, hrecv_sem, csend_sem, crecv_sem, zsend_sem, zrecv_sem,
             note_sem, ready_sem, far_sem, hello_sem, zready_sem):
    me, grp = lax.axis_index("dev"), lax.axis_index("grp")
    core = lax.rem(me, 2)
    base = me - core
    partner = base + 1 - core
    chans, rows = t_ref.shape[1:]
    tile = tile_of(rows)
    pieces = cuts_of(rows)
    across, xs, ys, ds = chips(n)
    late = [flip(me, k) for k in late_flips(n)]

    def x_core(chip):
        return jnp.where((chip > across) & (lax.rem(chip // 2, across // 2 + 1) == 0), 0, 1)

    def y_core(chip):
        return jnp.where((chip <= across) & (chip > 0), 0, 1)

    def lead(chip):
        return jnp.where((chip == 0) & (grp == 0), 0, 1)

    def targets(k):
        chip = flip(base, k)
        return [chip + lead(chip), chip + 1 - lead(chip)]

    def signal(sem, **device):
        pl.semaphore_signal(sem, inc=1, device_id=device, device_id_type=MESH)

    barrier = pltpu.get_barrier_semaphore()

    @pl.when(core == lead(base))
    def _():
        for k in ys:
            signal(barrier, dev=flip(base, k) + y_core(flip(base, k)))
        for k in xs:
            signal(barrier, dev=flip(base, k) + x_core(flip(base, k)))

    @pl.when(core == 1)
    def _():
        signal(barrier, dev=base)

    @pl.when((me == 1) & (grp > 0))
    def _():
        signal(barrier, grp=grp - 1)

    def at(j, lo=0, size=rows):
        return pl.ds(pl.multiple_of(j * rows + lo, LANES), size)

    load = pltpu.make_async_copy(x_ref, x_vm, load_sem)

    def remote(src, dst, sems, device):
        return pltpu.make_async_remote_copy(
            src_ref=src, dst_ref=dst, send_sem=sems[0], recv_sem=sems[1],
            device_id=device, device_id_type=MESH)

    def direct(j, sem, lo, hi):
        remote(x_ref.at[:, at(j, lo, hi - lo)], t_ref.at[me, :, pl.ds(lo, hi - lo)],
               (send_sem, recv_sem.at[sem]), {"dev": j}).start()

    def hop(j, slot):
        remote(x_ref.at[:, at(j)], relay_vm.at[slot],
               (hsend_sem, hrecv_sem.at[slot]), {"dev": flip(me, ds[slot // 2] & across)}).start()

    def relay(j, slot, sem, lo, hi):
        source = flip(me, ds[slot // 2] & across)
        remote(relay_vm.at[slot, :, pl.ds(lo, hi - lo)], t_ref.at[source, :, pl.ds(lo, hi - lo)],
               (send_sem, recv_sem.at[sem]), {"dev": j}).start()

    x_blocks = [j for k in xs for j in targets(k)]
    y_blocks = [j for k in ys for j in targets(k)]
    d_blocks = [j for k in ds for j in targets(k)]

    half = rows // 2
    x_side, y_side = core == x_core(base), core == y_core(base)

    after = jnp.where((me == 1) & (grp < groups - 1), 1, 0)
    faced = jnp.where(x_side, len(xs), 0) + jnp.where(y_side, len(ys), 0)
    pl.semaphore_wait(barrier, faced + 1 - core + after)

    @pl.when(x_side)
    def _():
        direct(x_blocks[0], 1, 0, half)

    @pl.when(y_side)
    def _():
        direct(y_blocks[0], 0, 0, rows)

    load.start()

    @pl.when(core == 0)
    def _():
        signal(note_sem, dev=base + 1)

    @pl.when((me == 1) & (grp < groups - 1))
    def _():
        signal(hello_sem, grp=grp + 1)

    pl.semaphore_wait(note_sem, 1)

    @pl.when(core == 1)
    def _():
        signal(note_sem, dev=base)
        for k in [*xs, *ys]:
            signal(ready_sem, dev=targets(k)[0])

    pl.semaphore_wait(ready_sem, jnp.where(core == lead(base), len(xs) + len(ys), 1))

    @pl.when(core == lead(base))
    def _():
        signal(ready_sem, dev=partner)

    @pl.when(core == 1)
    def _():
        for k in xs:
            for j in targets(k):
                signal(far_sem, dev=j)

    for slot, j in enumerate(d_blocks):
        hop(j, slot)

    @pl.when(jnp.logical_not(y_side))
    def _():
        direct(y_blocks[0], 0, 0, rows)

    for j in [*y_blocks[1:], partner]:
        direct(j, 0, 0, rows)
    load.wait()

    shape = (2 * LANES, 2 * LANES)
    row = lax.rem(lax.broadcasted_iota(jnp.int32, shape, 0), LANES)
    col = lax.broadcasted_iota(jnp.int32, shape, 1)
    w_ref[...] = jnp.where((row < col) | (col >= LANES), 1.0, 0.0).astype(jnp.bfloat16)

    def range_total(j, total):
        give_vm[j] = total

        def one(i, acc):
            block = x_vm[:, at(j, i * tile, tile)]
            parts = [block[:, s * LANES:(s + 1) * LANES] for s in range(tile // LANES)]
            while len(parts) > 1:
                parts = [a + b for a, b in zip(parts[::2], parts[1::2])] + parts[len(parts) & ~1:]
            return acc + parts[0]

        acc = lax.fori_loop(0, rows // tile, one, jnp.zeros((chans, LANES), jnp.float32))
        return total + jnp.broadcast_to(jnp.sum(acc, axis=1, keepdims=True), acc.shape)

    total = lax.fori_loop(0, n, range_total, jnp.zeros((chans, LANES), jnp.float32))

    pl.semaphore_wait(far_sem, len(xs))

    @pl.when((me == 1) & (grp > 0))
    def _():
        pl.semaphore_wait(hello_sem, 1)
        signal(zready_sem, grp=grp - 1)

    @pl.when(grp < groups - 1)
    def _():
        pl.semaphore_wait(zready_sem, 1)

    @pl.when((me == 1) & (grp < groups - 1))
    def _():
        for k in range(1, n):
            signal(zready_sem, dev=flip(me, k))

    def pass_on():
        return remote(group_vm.at[1], group_vm.at[0], (zsend_sem, zrecv_sem), {"grp": grp + 1})

    @pl.when(grp == 0)
    def _():
        group_vm[0] = jnp.zeros_like(total)

    @pl.when(grp > 0)
    def _():
        pass_on().wait_recv()

    before = group_vm[0]
    group_vm[1] = before + total
    for j in range(n):
        give_vm[j] = give_vm[j] + before
    carry_vm[me] = give_vm[me]

    @pl.when(grp < groups - 1)
    def _():
        pass_on().start()

    for j in [partner, *y_blocks, *x_blocks, *d_blocks]:
        remote(give_vm.at[j], carry_vm.at[me], (csend_sem, crecv_sem), {"dev": j}).start()

    @pl.when(jnp.logical_not(x_side))
    def _():
        direct(x_blocks[0], 1, 0, half)

    for slot, j in enumerate(x_blocks):
        for i, (lo, hi) in enumerate(pieces):
            if slot or i:
                direct(j, 1 + i, lo, hi)

    def scan(blocks, lo, hi, runs):
        width = min(hi - lo, 4 * tile // len(blocks))

        def one(i, runs):
            start = lo + i * width
            tiles = [source[:, pl.ds(pl.multiple_of(offset + start, LANES), width)] for source, offset, _ in blocks]
            outs, runs = scan_tiles(tiles, w_ref, runs)
            for (_, _, dest), parts in zip(blocks, outs):
                for j, sums in enumerate(parts):
                    dest[:, pl.ds(pl.multiple_of(start + j * LANES, LANES), LANES)] = sums
            return tuple(runs)

        return lax.fori_loop(0, (hi - lo) // width, one, tuple(runs))

    def in_place(j):
        return t_ref.at[j], 0, t_ref.at[j]

    def arrived(sem, blocks, lo=0, hi=rows):
        span = t_ref.at[pl.ds(0, blocks), :, pl.ds(lo, hi - lo)]
        remote(span, span, (send_sem, recv_sem.at[sem]), {"dev": partner}).wait_recv()

    scan([(x_vm, me * rows, t_ref.at[me])], 0, rows, [carry_vm[me]])
    for slot in range(len(d_blocks)):
        remote(relay_vm.at[slot], relay_vm.at[slot], (hsend_sem, hrecv_sem.at[slot]), {"dev": partner}).wait_recv()
        j = targets(ds[slot // 2] & ~across)[slot % 2]
        for i, (lo, hi) in enumerate(pieces):
            relay(j, slot, 1 + i, lo, hi)

    gives = carry_vm.at[pl.ds(0, n - 1)]
    remote(gives, gives, (csend_sem, crecv_sem), {"dev": partner}).wait()
    arrived(0, 1 + len(y_blocks))
    scan([in_place(partner)], 0, rows, [carry_vm[partner]])
    for s in range(0, len(y_blocks), 2):
        pair = y_blocks[s:s + 2]
        scan([in_place(j) for j in pair], 0, rows, [carry_vm[j] for j in pair])

    for i, j in enumerate(late):
        run_ref[i] = carry_vm[j]
    for i, (lo, hi) in enumerate(pieces[:-1]):
        arrived(1 + i, len(late), lo, hi)
        for s in range(0, len(late), 4):
            four = late[s:s + 4]
            runs = scan([in_place(j) for j in four], lo, hi, [run_ref[s + r] for r in range(len(four))])
            for r, run in enumerate(runs):
                run_ref[s + r] = run

    @pl.when(grp < groups - 1)
    def _():
        pass_on().wait_send()

    remote(relay_vm, relay_vm, (hsend_sem, hrecv_sem.at[0]), {"dev": partner}).wait_send()
    sent = x_vm.at[:, pl.ds(0, (n - 1) * rows)]
    remote(sent, sent, (send_sem, recv_sem.at[0]), {"dev": partner}).wait_send()
    arrived(len(pieces), len(late), *pieces[-1])


def write(n, t_ref, run_ref, w_ref, out_ref, stage, sem):
    me = lax.axis_index("dev")
    rows = t_ref.shape[2]
    tile = tile_of(rows)
    late = late_flips(n)
    main, last = pl.ds(0, rows - tile), pl.ds(rows - tile, tile)

    for k in range(n):
        j = flip(me, k)
        if k in late:
            pltpu.make_async_copy(t_ref.at[j, :, main], out_ref.at[j, :, main], sem).start()
        else:
            pltpu.make_async_copy(t_ref.at[j], out_ref.at[j], sem).start()
    for s in range(0, len(late), 4):
        four = late[s:s + 4]
        outs, _ = scan_tiles([t_ref[flip(me, k), :, last] for k in four], w_ref, [run_ref[s + r] for r in range(len(four))])
        for r, (k, parts) in enumerate(zip(four, outs)):
            for j, sums in enumerate(parts):
                stage[s + r, :, pl.ds(j * LANES, LANES)] = sums
            pltpu.make_async_copy(stage.at[s + r], out_ref.at[flip(me, k), :, last], sem).start()
    pltpu.make_async_copy(t_ref, out_ref, sem).wait()


def solution(mesh):
    n, groups = mesh.shape["dev"], mesh.shape["grp"]
    assert n >= 8 and not n & (n - 1)

    def local(amounts):
        chans, length = amounts.shape
        rows = length // n
        tile = tile_of(rows)
        late = len(late_flips(n))
        relays = 2 * len(chips(n)[3])
        f32 = jnp.float32
        dma = pltpu.SemaphoreType.DMA
        regular = pltpu.SemaphoreType.REGULAR
        wide = (2 * LANES, 2 * LANES)
        table, run, weights = pl.pallas_call(
            functools.partial(exchange, n, groups),
            out_shape=[jax.ShapeDtypeStruct((n, chans, rows), f32),
                       jax.ShapeDtypeStruct((late, chans, LANES), f32),
                       jax.ShapeDtypeStruct(wide, jnp.bfloat16)],
            in_specs=[pl.BlockSpec(memory_space=pl.ANY)],
            out_specs=[pl.BlockSpec(memory_space=pltpu.VMEM)] * 3,
            scratch_shapes=[
                pltpu.VMEM((chans, length), f32),
                pltpu.VMEM((relays, chans, rows), f32),
                pltpu.VMEM((n, chans, LANES), f32),
                pltpu.VMEM((n, chans, LANES), f32),
                pltpu.VMEM((2, chans, LANES), f32),
                dma, dma, dma((1 + len(cuts_of(rows)),)), dma, dma((relays,)),
                dma, dma, dma, dma, regular, regular, regular, regular, regular,
            ],
            compiler_params=pltpu.CompilerParams(
                collective_id=0, has_side_effects=True, vmem_limit_bytes=VMEM_GRANT),
            name="exchange",
        )(amounts)
        out = pl.pallas_call(
            functools.partial(write, n),
            out_shape=jax.ShapeDtypeStruct((n, chans, rows), f32),
            in_specs=[pl.BlockSpec(memory_space=pltpu.VMEM)] * 3,
            out_specs=pl.BlockSpec(memory_space=pl.ANY),
            scratch_shapes=[pltpu.VMEM((late, chans, tile), f32), dma],
            compiler_params=pltpu.CompilerParams(vmem_limit_bytes=VMEM_GRANT),
            name="write",
        )(table, run, weights)
        return out.reshape(n * chans, rows)

    return jax.shard_map(
        local,
        mesh=mesh,
        in_specs=(P("dev", "grp"),),
        out_specs=P(None, ("grp", "dev")),
        check_vma=False,
    )
```

```python
import functools

import jax
import jax.numpy as jnp
from jax import lax
from jax.experimental import pallas as pl
from jax.experimental.pallas import tpu as pltpu
from jax.sharding import PartitionSpec as P

MESH = pl.DeviceIdType.MESH
LANES = 128
VMEM_GRANT = 46 << 20


def flip(me, k):
    other, bit = me, 1
    while bit <= k:
        if k & bit:
            other = other + bit - 2 * bit * lax.rem(me // bit, 2)
        bit *= 2
    return other


def chips(n):
    across = (1 << (n.bit_length() - 2) // 2) - 1 << 1
    flips = range(2, n, 2)
    xs = [k for k in flips if not k & ~across]
    ys = [k for k in flips if not k & across]
    ds = [k for k in flips if k & across and k & ~across]
    return across, xs, ys, ds


def late_flips(n):
    _, xs, _, ds = chips(n)
    return [k + core for k in [*xs, *ds] for core in (0, 1)]


def tile_of(rows):
    return min(rows // 8, 2048)


def cuts_of(rows):
    cuts = [0, rows // 2, 3 * rows // 4, rows - tile_of(rows), rows]
    return list(zip(cuts[:-1], cuts[1:]))


def scan_tiles(blocks, w_ref, runs):
    chans, width = blocks[0].shape
    steps = width // LANES
    stack = jnp.concatenate(
        [block[:, j * LANES:(j + 1) * LANES] for block in blocks for j in range(steps)], axis=0)
    high = stack.astype(jnp.bfloat16)
    rest = stack - high.astype(jnp.float32)
    mid = rest.astype(jnp.bfloat16)
    low = (rest - mid.astype(jnp.float32)).astype(jnp.bfloat16)
    sums = jnp.dot(jnp.concatenate([high, mid], axis=1), w_ref[...], preferred_element_type=jnp.float32)
    sums = sums + jnp.dot(low, w_ref[:LANES, :], preferred_element_type=jnp.float32)
    outs, after = [], []
    for i, run in enumerate(runs):
        parts = []
        for j in range(i * steps, (i + 1) * steps):
            part = sums[j * chans:(j + 1) * chans]
            parts.append(part[:, :LANES] + run)
            run = run + part[:, LANES:]
        outs.append(parts)
        after.append(run)
    return outs, after


def exchange(n, groups, x_ref, t_ref, run_ref, w_ref, x_vm, relay_vm, give_vm, carry_vm, group_vm,
             load_sem, send_sem, recv_sem, hsend_sem, hrecv_sem, csend_sem, crecv_sem, zsend_sem, zrecv_sem,
             note_sem, ready_sem, far_sem, hello_sem, zready_sem):
    me, grp = lax.axis_index("dev"), lax.axis_index("grp")
    core = lax.rem(me, 2)
    base = me - core
    partner = base + 1 - core
    chans, rows = t_ref.shape[1:]
    tile = tile_of(rows)
    pieces = cuts_of(rows)
    across, xs, ys, ds = chips(n)
    late = [flip(me, k) for k in late_flips(n)]

    def x_core(chip):
        return jnp.where((chip > across) & (lax.rem(chip // 2, across // 2 + 1) == 0), 0, 1)

    def y_core(chip):
        return jnp.where((chip <= across) & (chip > 0), 0, 1)

    def lead(chip):
        return jnp.where((chip == 0) & (grp == 0), 0, 1)

    def targets(k):
        chip = flip(base, k)
        first = jnp.where((chip == 0) & (grp == 0), 0, core)
        return [chip + first, chip + 1 - first]

    def front(k):
        return flip(base, k) + lead(flip(base, k))

    def signal(sem, **device):
        pl.semaphore_signal(sem, inc=1, device_id=device, device_id_type=MESH)

    barrier = pltpu.get_barrier_semaphore()

    @pl.when(core == lead(base))
    def _():
        for k in ys:
            signal(barrier, dev=flip(base, k) + y_core(flip(base, k)))
        for k in xs:
            signal(barrier, dev=flip(base, k) + x_core(flip(base, k)))

    @pl.when(core == 1)
    def _():
        signal(barrier, dev=base)

    @pl.when((me == 1) & (grp > 0))
    def _():
        signal(barrier, grp=grp - 1)

    def at(j, lo=0, size=rows):
        return pl.ds(pl.multiple_of(j * rows + lo, LANES), size)

    load = pltpu.make_async_copy(x_ref, x_vm, load_sem)

    def remote(src, dst, sems, device):
        return pltpu.make_async_remote_copy(
            src_ref=src, dst_ref=dst, send_sem=sems[0], recv_sem=sems[1],
            device_id=device, device_id_type=MESH)

    def direct(j, sem, lo, hi):
        remote(x_ref.at[:, at(j, lo, hi - lo)], t_ref.at[me, :, pl.ds(lo, hi - lo)],
               (send_sem, recv_sem.at[sem]), {"dev": j}).start()

    def hop(j, slot):
        remote(x_ref.at[:, at(j)], relay_vm.at[slot],
               (hsend_sem, hrecv_sem.at[slot]), {"dev": flip(me, ds[slot // 2] & across)}).start()

    def relay(j, slot, sem, lo, hi):
        source = flip(me, ds[slot // 2] & across)
        remote(relay_vm.at[slot, :, pl.ds(lo, hi - lo)], t_ref.at[source, :, pl.ds(lo, hi - lo)],
               (send_sem, recv_sem.at[sem]), {"dev": j}).start()

    x_blocks = [j for k in xs for j in targets(k)]
    y_blocks = [j for k in ys for j in targets(k)]
    d_blocks = [j for k in ds for j in targets(k)]

    head = 3 * rows // 8
    x_side, y_side = core == x_core(base), core == y_core(base)

    after = jnp.where((me == 1) & (grp < groups - 1), 1, 0)
    faced = jnp.where(x_side, len(xs), 0) + jnp.where(y_side, len(ys), 0)
    pl.semaphore_wait(barrier, faced + 1 - core + after)

    @pl.when(x_side)
    def _():
        direct(front(xs[0]), 1, 0, head)

    @pl.when(y_side)
    def _():
        direct(front(ys[0]), 0, 0, head)

    load.start()

    @pl.when(core == 0)
    def _():
        signal(note_sem, dev=base + 1)

    @pl.when((me == 1) & (grp < groups - 1))
    def _():
        signal(hello_sem, grp=grp + 1)

    pl.semaphore_wait(note_sem, 1)

    @pl.when(jnp.logical_not(x_side))
    def _():
        direct(front(xs[0]), 1, 0, head)

    @pl.when(jnp.logical_not(y_side))
    def _():
        direct(front(ys[0]), 0, 0, head)

    def unopened(slot, opened, j, sem):
        if slot > 1:
            direct(j, sem, 0, head)
        else:
            @pl.when(j != opened)
            def _():
                direct(j, sem, 0, head)

    @pl.when(core == 1)
    def _():
        signal(note_sem, dev=base)
        for k in [*xs, *ys]:
            signal(ready_sem, dev=front(k))

    pl.semaphore_wait(ready_sem, jnp.where(core == lead(base), len(xs) + len(ys), 1))

    @pl.when(core == lead(base))
    def _():
        signal(ready_sem, dev=partner)

    @pl.when(core == 1)
    def _():
        for k in xs:
            for j in targets(k):
                signal(far_sem, dev=j)

    for slot, j in enumerate(d_blocks):
        hop(j, slot)
    for slot, j in enumerate(y_blocks):
        unopened(slot, front(ys[0]), j, 0)
        direct(j, 0, head, rows)
    direct(partner, 0, 0, rows)
    load.wait()

    shape = (2 * LANES, 2 * LANES)
    row = lax.rem(lax.broadcasted_iota(jnp.int32, shape, 0), LANES)
    col = lax.broadcasted_iota(jnp.int32, shape, 1)
    w_ref[...] = jnp.where((row < col) | (col >= LANES), 1.0, 0.0).astype(jnp.bfloat16)

    def range_total(j, total):
        give_vm[j] = total

        def one(i, acc):
            block = x_vm[:, at(j, i * tile, tile)]
            parts = [block[:, s * LANES:(s + 1) * LANES] for s in range(tile // LANES)]
            while len(parts) > 1:
                parts = [a + b for a, b in zip(parts[::2], parts[1::2])] + parts[len(parts) & ~1:]
            return acc + parts[0]

        acc = lax.fori_loop(0, rows // tile, one, jnp.zeros((chans, LANES), jnp.float32))
        return total + jnp.broadcast_to(jnp.sum(acc, axis=1, keepdims=True), acc.shape)

    total = lax.fori_loop(0, n, range_total, jnp.zeros((chans, LANES), jnp.float32))

    pl.semaphore_wait(far_sem, len(xs))

    @pl.when((me == 1) & (grp > 0))
    def _():
        pl.semaphore_wait(hello_sem, 1)
        signal(zready_sem, grp=grp - 1)

    @pl.when(grp < groups - 1)
    def _():
        pl.semaphore_wait(zready_sem, 1)

    @pl.when((me == 1) & (grp < groups - 1))
    def _():
        for k in range(1, n):
            signal(zready_sem, dev=flip(me, k))

    def pass_on():
        return remote(group_vm.at[1], group_vm.at[0], (zsend_sem, zrecv_sem), {"grp": grp + 1})

    @pl.when(grp == 0)
    def _():
        group_vm[0] = jnp.zeros_like(total)

    @pl.when(grp > 0)
    def _():
        pass_on().wait_recv()

    before = group_vm[0]
    group_vm[1] = before + total
    for j in range(n):
        give_vm[j] = give_vm[j] + before
    carry_vm[me] = give_vm[me]

    @pl.when(grp < groups - 1)
    def _():
        pass_on().start()

    for j in [partner, *y_blocks, *x_blocks, *d_blocks]:
        remote(give_vm.at[j], carry_vm.at[me], (csend_sem, crecv_sem), {"dev": j}).start()

    def scan(blocks, lo, hi, runs):
        width = min(hi - lo, 4 * tile // len(blocks))

        def one(i, runs):
            start = lo + i * width
            tiles = [source[:, pl.ds(pl.multiple_of(offset + start, LANES), width)] for source, offset, _ in blocks]
            outs, runs = scan_tiles(tiles, w_ref, runs)
            for (_, _, dest), parts in zip(blocks, outs):
                for j, sums in enumerate(parts):
                    dest[:, pl.ds(pl.multiple_of(start + j * LANES, LANES), LANES)] = sums
            return tuple(runs)

        return lax.fori_loop(0, (hi - lo) // width, one, tuple(runs))

    def in_place(j):
        return t_ref.at[j], 0, t_ref.at[j]

    def arrived(sem, blocks, lo=0, hi=rows):
        span = t_ref.at[pl.ds(0, blocks), :, pl.ds(lo, hi - lo)]
        remote(span, span, (send_sem, recv_sem.at[sem]), {"dev": partner}).wait_recv()

    scan([(x_vm, me * rows, t_ref.at[me])], 0, rows, [carry_vm[me]])
    for slot, j in enumerate(x_blocks):
        unopened(slot, front(xs[0]), j, 1)
        for i, (lo, hi) in enumerate(pieces):
            direct(j, 1 + i, lo if i else head, hi)

    for slot in range(len(d_blocks)):
        remote(relay_vm.at[slot], relay_vm.at[slot], (hsend_sem, hrecv_sem.at[slot]), {"dev": partner}).wait_recv()
        j = targets(ds[slot // 2] & ~across)[slot % 2]
        for i, (lo, hi) in enumerate(pieces):
            relay(j, slot, 1 + i, lo, hi)

    gives = carry_vm.at[pl.ds(0, n - 1)]
    remote(gives, gives, (csend_sem, crecv_sem), {"dev": partner}).wait()
    arrived(0, 1 + len(y_blocks))
    scan([in_place(partner)], 0, rows, [carry_vm[partner]])
    for s in range(0, len(y_blocks), 2):
        pair = y_blocks[s:s + 2]
        scan([in_place(j) for j in pair], 0, rows, [carry_vm[j] for j in pair])

    for i, j in enumerate(late):
        run_ref[i] = carry_vm[j]
    for i, (lo, hi) in enumerate(pieces[:-1]):
        arrived(1 + i, len(late), lo, hi)
        for s in range(0, len(late), 4):
            four = late[s:s + 4]
            runs = scan([in_place(j) for j in four], lo, hi, [run_ref[s + r] for r in range(len(four))])
            for r, run in enumerate(runs):
                run_ref[s + r] = run

    @pl.when(grp < groups - 1)
    def _():
        pass_on().wait_send()

    remote(relay_vm, relay_vm, (hsend_sem, hrecv_sem.at[0]), {"dev": partner}).wait_send()
    sent = x_vm.at[:, pl.ds(0, (n - 1) * rows)]
    remote(sent, sent, (send_sem, recv_sem.at[0]), {"dev": partner}).wait_send()
    arrived(len(pieces), len(late), *pieces[-1])


def write(n, t_ref, run_ref, w_ref, out_ref, stage, sem):
    me = lax.axis_index("dev")
    rows = t_ref.shape[2]
    tile = tile_of(rows)
    late = late_flips(n)
    main, last = pl.ds(0, rows - tile), pl.ds(rows - tile, tile)

    for k in range(n):
        j = flip(me, k)
        if k in late:
            pltpu.make_async_copy(t_ref.at[j, :, main], out_ref.at[j, :, main], sem).start()
        else:
            pltpu.make_async_copy(t_ref.at[j], out_ref.at[j], sem).start()
    for s in range(0, len(late), 4):
        four = late[s:s + 4]
        outs, _ = scan_tiles([t_ref[flip(me, k), :, last] for k in four], w_ref, [run_ref[s + r] for r in range(len(four))])
        for r, (k, parts) in enumerate(zip(four, outs)):
            for j, sums in enumerate(parts):
                stage[s + r, :, pl.ds(j * LANES, LANES)] = sums
            pltpu.make_async_copy(stage.at[s + r], out_ref.at[flip(me, k), :, last], sem).start()
    pltpu.make_async_copy(t_ref, out_ref, sem).wait()


def solution(mesh):
    n, groups = mesh.shape["dev"], mesh.shape["grp"]
    assert n >= 8 and not n & (n - 1)

    def local(amounts):
        chans, length = amounts.shape
        rows = length // n
        tile = tile_of(rows)
        late = len(late_flips(n))
        relays = 2 * len(chips(n)[3])
        f32 = jnp.float32
        dma = pltpu.SemaphoreType.DMA
        regular = pltpu.SemaphoreType.REGULAR
        wide = (2 * LANES, 2 * LANES)
        table, run, weights = pl.pallas_call(
            functools.partial(exchange, n, groups),
            out_shape=[jax.ShapeDtypeStruct((n, chans, rows), f32),
                       jax.ShapeDtypeStruct((late, chans, LANES), f32),
                       jax.ShapeDtypeStruct(wide, jnp.bfloat16)],
            in_specs=[pl.BlockSpec(memory_space=pl.ANY)],
            out_specs=[pl.BlockSpec(memory_space=pltpu.VMEM)] * 3,
            scratch_shapes=[
                pltpu.VMEM((chans, length), f32),
                pltpu.VMEM((relays, chans, rows), f32),
                pltpu.VMEM((n, chans, LANES), f32),
                pltpu.VMEM((n, chans, LANES), f32),
                pltpu.VMEM((2, chans, LANES), f32),
                dma, dma, dma((1 + len(cuts_of(rows)),)), dma, dma((relays,)),
                dma, dma, dma, dma, regular, regular, regular, regular, regular,
            ],
            compiler_params=pltpu.CompilerParams(
                collective_id=0, has_side_effects=True, vmem_limit_bytes=VMEM_GRANT),
            name="exchange",
        )(amounts)
        out = pl.pallas_call(
            functools.partial(write, n),
            out_shape=jax.ShapeDtypeStruct((n, chans, rows), f32),
            in_specs=[pl.BlockSpec(memory_space=pltpu.VMEM)] * 3,
            out_specs=pl.BlockSpec(memory_space=pl.ANY),
            scratch_shapes=[pltpu.VMEM((late, chans, tile), f32), dma],
            compiler_params=pltpu.CompilerParams(vmem_limit_bytes=VMEM_GRANT),
            name="write",
        )(table, run, weights)
        return out.reshape(n * chans, rows)

    return jax.shard_map(
        local,
        mesh=mesh,
        in_specs=(P("dev", "grp"),),
        out_specs=P(None, ("grp", "dev")),
        check_vma=False,
    )
```

```python
import functools

import jax
import jax.numpy as jnp
from jax import lax
from jax.experimental import pallas as pl
from jax.experimental.pallas import tpu as pltpu
from jax.sharding import PartitionSpec as P

MESH = pl.DeviceIdType.MESH
LANES = 128
VMEM_GRANT = 46 << 20


def flip(me, k):
    other, bit = me, 1
    while bit <= k:
        if k & bit:
            other = other + bit - 2 * bit * lax.rem(me // bit, 2)
        bit *= 2
    return other


def chips(n):
    across = (1 << (n.bit_length() - 2) // 2) - 1 << 1
    flips = range(2, n, 2)
    xs = [k for k in flips if not k & ~across]
    ys = [k for k in flips if not k & across]
    ds = [k for k in flips if k & across and k & ~across]
    return across, xs, ys, ds


def late_flips(n):
    _, xs, _, ds = chips(n)
    return [k + core for k in [*xs, *ds] for core in (0, 1)]


def tile_of(rows):
    return min(rows // 8, 2048)


def cuts_of(rows):
    cuts = [0, rows // 2, 3 * rows // 4, rows - tile_of(rows), rows]
    return list(zip(cuts[:-1], cuts[1:]))


def scan_tiles(blocks, w_ref, runs):
    chans, width = blocks[0].shape
    steps = width // LANES
    stack = jnp.concatenate(
        [block[:, j * LANES:(j + 1) * LANES] for block in blocks for j in range(steps)], axis=0)
    high = stack.astype(jnp.bfloat16)
    rest = stack - high.astype(jnp.float32)
    mid = rest.astype(jnp.bfloat16)
    low = (rest - mid.astype(jnp.float32)).astype(jnp.bfloat16)
    sums = jnp.dot(jnp.concatenate([high, mid], axis=1), w_ref[...], preferred_element_type=jnp.float32)
    sums = sums + jnp.dot(low, w_ref[:LANES, :], preferred_element_type=jnp.float32)
    outs, after = [], []
    for i, run in enumerate(runs):
        parts = []
        for j in range(i * steps, (i + 1) * steps):
            part = sums[j * chans:(j + 1) * chans]
            parts.append(part[:, :LANES] + run)
            run = run + part[:, LANES:]
        outs.append(parts)
        after.append(run)
    return outs, after


def last_lane(tile):
    return jnp.broadcast_to(tile[:, LANES - 1:], tile.shape)


def exchange(n, groups, x_ref, t_ref, run_ref, w_ref, x_vm, relay_vm, give_vm, carry_vm, group_vm,
             load_sem, send_sem, recv_sem, hsend_sem, hrecv_sem, csend_sem, crecv_sem, zsend_sem, zrecv_sem,
             note_sem, ready_sem, far_sem, hello_sem, zready_sem):
    me, grp = lax.axis_index("dev"), lax.axis_index("grp")
    core = lax.rem(me, 2)
    base = me - core
    partner = base + 1 - core
    chans, rows = t_ref.shape[1:]
    tile = tile_of(rows)
    pieces = cuts_of(rows)
    across, xs, ys, ds = chips(n)
    late = [flip(me, k) for k in late_flips(n)]

    def x_core(chip):
        return jnp.where((chip > across) & (lax.rem(chip // 2, across // 2 + 1) == 0), 0, 1)

    def y_core(chip):
        return jnp.where((chip <= across) & (chip > 0), 0, 1)

    def lead(chip):
        return jnp.where((chip == 0) & (grp == 0), 0, 1)

    def targets(k):
        chip = flip(base, k)
        return [chip + lead(chip), chip + 1 - lead(chip)]

    def signal(sem, **device):
        pl.semaphore_signal(sem, inc=1, device_id=device, device_id_type=MESH)

    barrier = pltpu.get_barrier_semaphore()

    @pl.when(core == lead(base))
    def _():
        for k in ys:
            signal(barrier, dev=flip(base, k) + y_core(flip(base, k)))
        for k in xs:
            signal(barrier, dev=flip(base, k) + x_core(flip(base, k)))

    @pl.when(core == 1)
    def _():
        signal(barrier, dev=base)

    @pl.when((me == 1) & (grp > 0))
    def _():
        signal(barrier, grp=grp - 1)

    def at(j, lo=0, size=rows):
        return pl.ds(pl.multiple_of(j * rows + lo, LANES), size)

    load = pltpu.make_async_copy(x_ref, x_vm, load_sem)

    def remote(src, dst, sems, device):
        return pltpu.make_async_remote_copy(
            src_ref=src, dst_ref=dst, send_sem=sems[0], recv_sem=sems[1],
            device_id=device, device_id_type=MESH)

    def direct(j, sem, lo, hi, source=x_ref):
        remote(source.at[:, at(j, lo, hi - lo)], t_ref.at[me, :, pl.ds(lo, hi - lo)],
               (send_sem, recv_sem.at[sem]), {"dev": j}).start()

    def hop(j, slot, part, source):
        lo, hi = parts[part]
        remote(source.at[:, at(j, lo, hi - lo)], relay_vm.at[slot, :, pl.ds(lo, hi - lo)],
               (hsend_sem, hrecv_sem.at[slot, part]), {"dev": flip(me, ds[slot // 2] & across)}).start()

    def relay(j, slot, sem, lo, hi):
        source = flip(me, ds[slot // 2] & across)
        remote(relay_vm.at[slot, :, pl.ds(lo, hi - lo)], t_ref.at[source, :, pl.ds(lo, hi - lo)],
               (send_sem, recv_sem.at[sem]), {"dev": j}).start()

    x_blocks = [j for k in xs for j in targets(k)]
    y_blocks = [j for k in ys for j in targets(k)]
    d_blocks = [j for k in ds for j in targets(k)]

    half = rows // 2
    main = rows - tile
    parts = [(0, main), (main, rows)]
    x_side, y_side = core == x_core(base), core == y_core(base)

    after = jnp.where((me == 1) & (grp < groups - 1), 1, 0)
    faced = jnp.where(x_side, len(xs), 0) + jnp.where(y_side, len(ys), 0)
    pl.semaphore_wait(barrier, faced + 1 - core + after)

    @pl.when(x_side)
    def _():
        direct(x_blocks[0], 1, 0, half)

    @pl.when(y_side)
    def _():
        direct(y_blocks[0], 0, 0, main)

    load.start()

    @pl.when(core == 0)
    def _():
        signal(note_sem, dev=base + 1)

    @pl.when((me == 1) & (grp < groups - 1))
    def _():
        signal(hello_sem, grp=grp + 1)

    pl.semaphore_wait(note_sem, 1)

    @pl.when(core == 1)
    def _():
        signal(note_sem, dev=base)
        for k in [*xs, *ys]:
            signal(ready_sem, dev=targets(k)[0])

    pl.semaphore_wait(ready_sem, jnp.where(core == lead(base), len(xs) + len(ys), 1))

    @pl.when(core == lead(base))
    def _():
        signal(ready_sem, dev=partner)

    @pl.when(core == 1)
    def _():
        for k in xs:
            for j in targets(k):
                signal(far_sem, dev=j)

    for slot, j in enumerate(d_blocks):
        hop(j, slot, 0, x_ref)

    @pl.when(jnp.logical_not(y_side))
    def _():
        direct(y_blocks[0], 0, 0, main)

    for j in y_blocks[1:]:
        direct(j, 0, 0, main)
    direct(partner, 0, 0, rows)
    load.wait()

    shape = (2 * LANES, 2 * LANES)
    row = lax.rem(lax.broadcasted_iota(jnp.int32, shape, 0), LANES)
    col = lax.broadcasted_iota(jnp.int32, shape, 1)
    w_ref[...] = jnp.where((row < col) | (col >= LANES), 1.0, 0.0).astype(jnp.bfloat16)

    def range_total(j, total):
        give_vm[j] = total

        def one(i, acc):
            block = x_vm[:, at(j, i * tile, tile)]
            parts = [block[:, s * LANES:(s + 1) * LANES] for s in range(tile // LANES)]
            while len(parts) > 1:
                parts = [a + b for a, b in zip(parts[::2], parts[1::2])] + parts[len(parts) & ~1:]
            return acc + parts[0]

        acc = lax.fori_loop(0, rows // tile, one, jnp.zeros((chans, LANES), jnp.float32))
        return total + jnp.broadcast_to(jnp.sum(acc, axis=1, keepdims=True), acc.shape)

    total = lax.fori_loop(0, n, range_total, jnp.zeros((chans, LANES), jnp.float32))

    pl.semaphore_wait(far_sem, len(xs))

    @pl.when((me == 1) & (grp > 0))
    def _():
        pl.semaphore_wait(hello_sem, 1)
        signal(zready_sem, grp=grp - 1)

    @pl.when(grp < groups - 1)
    def _():
        pl.semaphore_wait(zready_sem, 1)

    @pl.when((me == 1) & (grp < groups - 1))
    def _():
        for k in range(1, n):
            signal(zready_sem, dev=flip(me, k))

    def pass_on():
        return remote(group_vm.at[1], group_vm.at[0], (zsend_sem, zrecv_sem), {"grp": grp + 1})

    @pl.when(grp == 0)
    def _():
        group_vm[0] = jnp.zeros_like(total)

    @pl.when(grp > 0)
    def _():
        pass_on().wait_recv()

    before = group_vm[0]
    group_vm[1] = before + total
    for j in range(n):
        give_vm[j] = give_vm[j] + before
    carry_vm[me] = give_vm[me]

    @pl.when(grp < groups - 1)
    def _():
        pass_on().start()

    lane = lax.broadcasted_iota(jnp.int32, (chans, LANES), 1)
    for j in range(n):
        end = pl.ds((j + 1) * rows - LANES, LANES)
        x_vm[:, end] = jnp.where(lane == LANES - 1, give_vm[j], x_vm[:, end])
    given = remote(give_vm.at[partner], carry_vm.at[me], (csend_sem, crecv_sem), {"dev": partner})
    given.start()
    for slot, j in enumerate(d_blocks):
        hop(j, slot, 1, x_vm)
    for j in y_blocks:
        direct(j, 0, main, rows, x_vm)

    @pl.when(jnp.logical_not(x_side))
    def _():
        direct(x_blocks[0], 1, 0, half)

    for slot, j in enumerate(x_blocks):
        for i, (lo, hi) in enumerate(pieces):
            if slot or i:
                direct(j, 1 + i, lo, hi, x_vm if hi == rows else x_ref)

    def scan(blocks, lo, hi, runs):
        width = min(hi - lo, 4 * tile // len(blocks))

        def one(i, runs):
            start = lo + i * width
            tiles = [source[:, pl.ds(pl.multiple_of(offset + start, LANES), width)] for source, offset, _ in blocks]
            outs, runs = scan_tiles(tiles, w_ref, runs)
            for (_, _, dest), parts in zip(blocks, outs):
                for j, sums in enumerate(parts):
                    dest[:, pl.ds(pl.multiple_of(start + j * LANES, LANES), LANES)] = sums
            return tuple(runs)

        return lax.fori_loop(0, (hi - lo) // width, one, tuple(runs))

    def in_place(j):
        return t_ref.at[j], 0, t_ref.at[j]

    def arrived(sem, blocks, lo=0, hi=rows):
        span = t_ref.at[pl.ds(0, blocks), :, pl.ds(lo, hi - lo)]
        remote(span, span, (send_sem, recv_sem.at[sem]), {"dev": partner}).wait_recv()

    scan([(x_vm, me * rows, t_ref.at[me])], 0, rows, [carry_vm[me]])
    def forward(slot, part):
        lo, hi = parts[part]
        span = relay_vm.at[slot, :, pl.ds(lo, hi - lo)]
        remote(span, span, (hsend_sem, hrecv_sem.at[slot, part]), {"dev": partner}).wait_recv()
        j = targets(ds[slot // 2] & ~across)[slot % 2]
        for i, (start, end) in enumerate(pieces):
            if lo <= start < hi:
                relay(j, slot, 1 + i, start, end)

    for slot in range(len(d_blocks)):
        forward(slot, 0)
    for slot in range(len(d_blocks)):
        forward(slot, 1)

    given.wait()
    arrived(0, 1 + len(y_blocks))
    scan([in_place(partner)], 0, rows, [carry_vm[partner]])
    for s in range(0, len(y_blocks), 2):
        pair = y_blocks[s:s + 2]
        runs = [last_lane(t_ref[j, :, pl.ds(rows - LANES, LANES)]) for j in pair]
        scan([in_place(j) for j in pair], 0, rows, runs)

    for i in range(len(late)):
        run_ref[i] = jnp.zeros((chans, LANES), jnp.float32)
    for i, (lo, hi) in enumerate(pieces[:-1]):
        arrived(1 + i, len(late), lo, hi)
        for s in range(0, len(late), 4):
            four = late[s:s + 4]
            runs = scan([in_place(j) for j in four], lo, hi, [run_ref[s + r] for r in range(len(four))])
            for r, run in enumerate(runs):
                run_ref[s + r] = run

    @pl.when(grp < groups - 1)
    def _():
        pass_on().wait_send()

    remote(relay_vm, relay_vm, (hsend_sem, hrecv_sem.at[0, 0]), {"dev": partner}).wait_send()
    sent = x_vm.at[:, pl.ds(0, (n - 1) * rows)]
    remote(sent, sent, (send_sem, recv_sem.at[0]), {"dev": partner}).wait_send()
    arrived(len(pieces), len(late), *pieces[-1])


def write(n, t_ref, run_ref, w_ref, out_ref, stage, sem):
    me = lax.axis_index("dev")
    rows = t_ref.shape[2]
    tile = tile_of(rows)
    late = late_flips(n)
    last = pl.ds(rows - tile, tile)

    for k in range(n):
        if k not in late:
            j = flip(me, k)
            pltpu.make_async_copy(t_ref.at[j], out_ref.at[j], sem).start()
    for s in range(0, len(late), 4):
        four = [flip(me, k) for k in late[s:s + 4]]
        carries = [last_lane(t_ref[j, :, pl.ds(rows - LANES, LANES)]) for j in four]
        runs = [run_ref[s + r] + carry for r, carry in enumerate(carries)]
        outs, _ = scan_tiles([t_ref[j, :, last] for j in four], w_ref, runs)
        for r, (j, carry, parts) in enumerate(zip(four, carries, outs)):
            wide = jnp.concatenate([carry] * (tile // LANES), axis=1)

            def add(i, _):
                at = pl.ds(pl.multiple_of(i * tile, LANES), tile)
                stage[s + r, :, at] = t_ref[j, :, at] + wide
                return 0

            lax.fori_loop(0, rows // tile - 1, add, 0, unroll=True)
            for i, sums in enumerate(parts):
                stage[s + r, :, pl.ds(rows - tile + i * LANES, LANES)] = sums
            pltpu.make_async_copy(stage.at[s + r], out_ref.at[j], sem).start()
    pltpu.make_async_copy(t_ref, out_ref, sem).wait()


def solution(mesh):
    n, groups = mesh.shape["dev"], mesh.shape["grp"]
    assert n >= 8 and not n & (n - 1)

    def local(amounts):
        chans, length = amounts.shape
        rows = length // n
        late = len(late_flips(n))
        relays = 2 * len(chips(n)[3])
        f32 = jnp.float32
        dma = pltpu.SemaphoreType.DMA
        regular = pltpu.SemaphoreType.REGULAR
        wide = (2 * LANES, 2 * LANES)
        table, run, weights = pl.pallas_call(
            functools.partial(exchange, n, groups),
            out_shape=[jax.ShapeDtypeStruct((n, chans, rows), f32),
                       jax.ShapeDtypeStruct((late, chans, LANES), f32),
                       jax.ShapeDtypeStruct(wide, jnp.bfloat16)],
            in_specs=[pl.BlockSpec(memory_space=pl.ANY)],
            out_specs=[pl.BlockSpec(memory_space=pltpu.VMEM)] * 3,
            scratch_shapes=[
                pltpu.VMEM((chans, length), f32),
                pltpu.VMEM((relays, chans, rows), f32),
                pltpu.VMEM((n, chans, LANES), f32),
                pltpu.VMEM((n, chans, LANES), f32),
                pltpu.VMEM((2, chans, LANES), f32),
                dma, dma, dma((1 + len(cuts_of(rows)),)), dma, dma((relays, 2)),
                dma, dma, dma, dma, regular, regular, regular, regular, regular,
            ],
            compiler_params=pltpu.CompilerParams(
                collective_id=0, has_side_effects=True, vmem_limit_bytes=VMEM_GRANT),
            name="exchange",
        )(amounts)
        out = pl.pallas_call(
            functools.partial(write, n),
            out_shape=jax.ShapeDtypeStruct((n, chans, rows), f32),
            in_specs=[pl.BlockSpec(memory_space=pltpu.VMEM)] * 3,
            out_specs=pl.BlockSpec(memory_space=pl.ANY),
            scratch_shapes=[pltpu.VMEM((late, chans, rows), f32), dma],
            compiler_params=pltpu.CompilerParams(vmem_limit_bytes=VMEM_GRANT),
            name="write",
        )(table, run, weights)
        return out.reshape(n * chans, rows)

    return jax.shard_map(
        local,
        mesh=mesh,
        in_specs=(P("dev", "grp"),),
        out_specs=P(None, ("grp", "dev")),
        check_vma=False,
    )
```

```python
import functools

import jax
import jax.numpy as jnp
from jax import lax
from jax.experimental import pallas as pl
from jax.experimental.pallas import tpu as pltpu
from jax.sharding import PartitionSpec as P

MESH = pl.DeviceIdType.MESH
LANES = 128
VMEM_GRANT = 46 << 20


def flip(me, k):
    other, bit = me, 1
    while bit <= k:
        if k & bit:
            other = other + bit - 2 * bit * lax.rem(me // bit, 2)
        bit *= 2
    return other


def chips(n):
    across = (1 << (n.bit_length() - 2) // 2) - 1 << 1
    flips = range(2, n, 2)
    xs = [k for k in flips if not k & ~across]
    ys = [k for k in flips if not k & across]
    ds = [k for k in flips if k & across and k & ~across]
    return across, xs, ys, ds


def late_flips(n):
    _, xs, _, ds = chips(n)
    return [k + core for k in [*xs, *ds] for core in (0, 1)]


def tile_of(rows):
    return min(rows // 8, 2048)


def cuts_of(rows):
    cuts = [0, rows // 2, 3 * rows // 4, rows - tile_of(rows), rows]
    return list(zip(cuts[:-1], cuts[1:]))


def scan_tiles(blocks, w_ref, runs):
    chans, width = blocks[0].shape
    steps = width // LANES
    stack = jnp.concatenate(
        [block[:, j * LANES:(j + 1) * LANES] for block in blocks for j in range(steps)], axis=0)
    high = stack.astype(jnp.bfloat16)
    rest = stack - high.astype(jnp.float32)
    mid = rest.astype(jnp.bfloat16)
    low = (rest - mid.astype(jnp.float32)).astype(jnp.bfloat16)
    sums = jnp.dot(jnp.concatenate([high, mid], axis=1), w_ref[...], preferred_element_type=jnp.float32)
    sums = sums + jnp.dot(low, w_ref[:LANES, :], preferred_element_type=jnp.float32)
    outs, after = [], []
    for i, run in enumerate(runs):
        parts = []
        for j in range(i * steps, (i + 1) * steps):
            part = sums[j * chans:(j + 1) * chans]
            parts.append(part[:, :LANES] + run)
            run = run + part[:, LANES:]
        outs.append(parts)
        after.append(run)
    return outs, after


def last_lane(tile):
    return jnp.broadcast_to(tile[:, LANES - 1:], tile.shape)


def exchange(n, groups, x_ref, t_ref, run_ref, w_ref, x_vm, relay_vm, give_vm, group_vm,
             load_sem, send_sem, recv_sem, hsend_sem, hrecv_sem, zsend_sem, zrecv_sem,
             note_sem, ready_sem, far_sem, hello_sem, zready_sem):
    me, grp = lax.axis_index("dev"), lax.axis_index("grp")
    core = lax.rem(me, 2)
    base = me - core
    partner = base + 1 - core
    chans, rows = t_ref.shape[1:]
    tile = tile_of(rows)
    pieces = cuts_of(rows)
    across, xs, ys, ds = chips(n)
    late = [flip(me, k) for k in late_flips(n)]

    def x_core(chip):
        return jnp.where((chip > across) & (lax.rem(chip // 2, across // 2 + 1) == 0), 0, 1)

    def y_core(chip):
        return jnp.where((chip <= across) & (chip > 0), 0, 1)

    def lead(chip):
        return jnp.where((chip == 0) & (grp == 0), 0, 1)

    def targets(k):
        chip = flip(base, k)
        return [chip + lead(chip), chip + 1 - lead(chip)]

    def signal(sem, **device):
        pl.semaphore_signal(sem, inc=1, device_id=device, device_id_type=MESH)

    barrier = pltpu.get_barrier_semaphore()

    @pl.when(core == lead(base))
    def _():
        for k in ys:
            signal(barrier, dev=flip(base, k) + y_core(flip(base, k)))
        for k in xs:
            signal(barrier, dev=flip(base, k) + x_core(flip(base, k)))

    @pl.when(core == 1)
    def _():
        signal(barrier, dev=base)

    @pl.when((me == 1) & (grp > 0))
    def _():
        signal(barrier, grp=grp - 1)

    def at(j, lo=0, size=rows):
        return pl.ds(pl.multiple_of(j * rows + lo, LANES), size)

    load = pltpu.make_async_copy(x_ref, x_vm, load_sem)

    def remote(src, dst, sems, device):
        return pltpu.make_async_remote_copy(
            src_ref=src, dst_ref=dst, send_sem=sems[0], recv_sem=sems[1],
            device_id=device, device_id_type=MESH)

    def direct(j, sem, lo, hi, source=x_ref):
        remote(source.at[:, at(j, lo, hi - lo)], t_ref.at[me, :, pl.ds(lo, hi - lo)],
               (send_sem, recv_sem.at[sem]), {"dev": j}).start()

    def hop(j, slot, part, source):
        lo, hi = parts[part]
        remote(source.at[:, at(j, lo, hi - lo)], relay_vm.at[slot, :, pl.ds(lo, hi - lo)],
               (hsend_sem, hrecv_sem.at[len(d_blocks) if part else slot]), {"dev": flip(me, ds[slot // 2] & across)}).start()

    def relay(j, slot, sem, lo, hi):
        source = flip(me, ds[slot // 2] & across)
        remote(relay_vm.at[slot, :, pl.ds(lo, hi - lo)], t_ref.at[source, :, pl.ds(lo, hi - lo)],
               (send_sem, recv_sem.at[sem]), {"dev": j}).start()

    x_blocks = [j for k in xs for j in targets(k)]
    y_blocks = [j for k in ys for j in targets(k)]
    d_blocks = [j for k in ds for j in targets(k)]

    half = rows // 2
    main = rows - tile
    parts = [(0, main), (main, rows)]
    x_side, y_side = core == x_core(base), core == y_core(base)

    after = jnp.where((me == 1) & (grp < groups - 1), 1, 0)
    faced = jnp.where(x_side, len(xs), 0) + jnp.where(y_side, len(ys), 0)
    pl.semaphore_wait(barrier, faced + 1 - core + after)

    @pl.when(x_side)
    def _():
        direct(x_blocks[0], 1, 0, half)

    @pl.when(y_side)
    def _():
        direct(y_blocks[0], 0, 0, main)

    load.start()

    @pl.when(core == 0)
    def _():
        signal(note_sem, dev=base + 1)

    @pl.when((me == 1) & (grp < groups - 1))
    def _():
        signal(hello_sem, grp=grp + 1)

    pl.semaphore_wait(note_sem, 1)

    @pl.when(core == 1)
    def _():
        signal(note_sem, dev=base)
        for k in [*xs, *ys]:
            signal(ready_sem, dev=targets(k)[0])

    pl.semaphore_wait(ready_sem, jnp.where(core == lead(base), len(xs) + len(ys), 1))

    @pl.when(core == lead(base))
    def _():
        signal(ready_sem, dev=partner)

    @pl.when(core == 1)
    def _():
        for k in xs:
            for j in targets(k):
                signal(far_sem, dev=j)

    for slot, j in enumerate(d_blocks):
        hop(j, slot, 0, x_ref)

    @pl.when(jnp.logical_not(y_side))
    def _():
        direct(y_blocks[0], 0, 0, main)

    for j in y_blocks[1:]:
        direct(j, 0, 0, main)
    direct(partner, 0, 0, main)
    load.wait()

    shape = (2 * LANES, 2 * LANES)
    row = lax.rem(lax.broadcasted_iota(jnp.int32, shape, 0), LANES)
    col = lax.broadcasted_iota(jnp.int32, shape, 1)
    w_ref[...] = jnp.where((row < col) | (col >= LANES), 1.0, 0.0).astype(jnp.bfloat16)

    def range_total(j, total):
        give_vm[j] = total

        def one(i, acc):
            block = x_vm[:, at(j, i * tile, tile)]
            parts = [block[:, s * LANES:(s + 1) * LANES] for s in range(tile // LANES)]
            while len(parts) > 1:
                parts = [a + b for a, b in zip(parts[::2], parts[1::2])] + parts[len(parts) & ~1:]
            return acc + parts[0]

        acc = lax.fori_loop(0, rows // tile, one, jnp.zeros((chans, LANES), jnp.float32))
        return total + jnp.broadcast_to(jnp.sum(acc, axis=1, keepdims=True), acc.shape)

    total = lax.fori_loop(0, n, range_total, jnp.zeros((chans, LANES), jnp.float32))

    pl.semaphore_wait(far_sem, len(xs))

    @pl.when((me == 1) & (grp > 0))
    def _():
        pl.semaphore_wait(hello_sem, 1)
        signal(zready_sem, grp=grp - 1)

    @pl.when(grp < groups - 1)
    def _():
        pl.semaphore_wait(zready_sem, 1)

    @pl.when((me == 1) & (grp < groups - 1))
    def _():
        for k in range(1, n):
            signal(zready_sem, dev=flip(me, k))

    def pass_on():
        return remote(group_vm.at[1], group_vm.at[0], (zsend_sem, zrecv_sem), {"grp": grp + 1})

    @pl.when(grp == 0)
    def _():
        group_vm[0] = jnp.zeros_like(total)

    @pl.when(grp > 0)
    def _():
        pass_on().wait_recv()

    before = group_vm[0]
    group_vm[1] = before + total
    for j in range(n):
        give_vm[j] = give_vm[j] + before

    @pl.when(grp < groups - 1)
    def _():
        pass_on().start()

    lane = lax.broadcasted_iota(jnp.int32, (chans, LANES), 1)
    for j in range(n):
        end = pl.ds((j + 1) * rows - LANES, LANES)
        x_vm[:, end] = jnp.where(lane == LANES - 1, give_vm[j], x_vm[:, end])
    direct(partner, 0, main, rows, x_vm)
    for slot, j in enumerate(d_blocks):
        hop(j, slot, 1, x_vm)
    for j in y_blocks:
        direct(j, 0, main, rows, x_vm)

    @pl.when(jnp.logical_not(x_side))
    def _():
        direct(x_blocks[0], 1, 0, half)

    for slot, j in enumerate(x_blocks):
        for i, (lo, hi) in enumerate(pieces):
            if slot or i:
                direct(j, 1 + i, lo, hi, x_vm if hi == rows else x_ref)

    def scan(blocks, lo, hi, runs):
        width = min(hi - lo, 4 * tile // len(blocks))

        def one(i, runs):
            start = lo + i * width
            tiles = [source[:, pl.ds(pl.multiple_of(offset + start, LANES), width)] for source, offset, _ in blocks]
            outs, runs = scan_tiles(tiles, w_ref, runs)
            for (_, _, dest), parts in zip(blocks, outs):
                for j, sums in enumerate(parts):
                    dest[:, pl.ds(pl.multiple_of(start + j * LANES, LANES), LANES)] = sums
            return tuple(runs)

        return lax.fori_loop(0, (hi - lo) // width, one, tuple(runs))

    def in_place(j):
        return t_ref.at[j], 0, t_ref.at[j]

    def arrived(sem, blocks, lo=0, hi=rows):
        span = t_ref.at[pl.ds(0, blocks), :, pl.ds(lo, hi - lo)]
        remote(span, span, (send_sem, recv_sem.at[sem]), {"dev": partner}).wait_recv()

    scan([(x_vm, me * rows, t_ref.at[me])], 0, rows, [give_vm[me]])
    def forward(slots, part):
        lo, hi = parts[part]
        span = relay_vm.at[pl.ds(slots[0], len(slots)), :, pl.ds(lo, hi - lo)]
        sem = hrecv_sem.at[len(d_blocks) if part else slots[0]]
        remote(span, span, (hsend_sem, sem), {"dev": partner}).wait_recv()
        for slot in slots:
            j = targets(ds[slot // 2] & ~across)[slot % 2]
            for i, (start, end) in enumerate(pieces):
                if lo <= start < hi:
                    relay(j, slot, 1 + i, start, end)

    for slot in range(len(d_blocks)):
        forward([slot], 0)
    forward(range(len(d_blocks)), 1)

    arrived(0, 1 + len(y_blocks))
    scan([in_place(partner)], 0, rows, [last_lane(t_ref[partner, :, pl.ds(rows - LANES, LANES)])])
    for s in range(0, len(y_blocks), 2):
        pair = y_blocks[s:s + 2]
        runs = [last_lane(t_ref[j, :, pl.ds(rows - LANES, LANES)]) for j in pair]
        scan([in_place(j) for j in pair], 0, rows, runs)

    for i in range(len(late)):
        run_ref[i] = jnp.zeros((chans, LANES), jnp.float32)
    for i, (lo, hi) in enumerate(pieces[:-1]):
        arrived(1 + i, len(late), lo, hi)
        for s in range(0, len(late), 4):
            four = late[s:s + 4]
            runs = scan([in_place(j) for j in four], lo, hi, [run_ref[s + r] for r in range(len(four))])
            for r, run in enumerate(runs):
                run_ref[s + r] = run

    @pl.when(grp < groups - 1)
    def _():
        pass_on().wait_send()

    remote(relay_vm, relay_vm, (hsend_sem, hrecv_sem.at[0]), {"dev": partner}).wait_send()
    sent = x_vm.at[:, pl.ds(0, (n - 1) * rows)]
    remote(sent, sent, (send_sem, recv_sem.at[0]), {"dev": partner}).wait_send()
    arrived(len(pieces), len(late), *pieces[-1])


def write(n, t_ref, run_ref, w_ref, out_ref, stage, sem):
    me = lax.axis_index("dev")
    rows = t_ref.shape[2]
    tile = tile_of(rows)
    late = late_flips(n)
    last = pl.ds(rows - tile, tile)

    for k in range(n):
        if k not in late:
            j = flip(me, k)
            pltpu.make_async_copy(t_ref.at[j], out_ref.at[j], sem).start()
    for s in range(0, len(late), 4):
        four = [flip(me, k) for k in late[s:s + 4]]
        carries = [last_lane(t_ref[j, :, pl.ds(rows - LANES, LANES)]) for j in four]
        runs = [run_ref[s + r] + carry for r, carry in enumerate(carries)]
        outs, _ = scan_tiles([t_ref[j, :, last] for j in four], w_ref, runs)
        for r, (j, carry, parts) in enumerate(zip(four, carries, outs)):
            wide = jnp.concatenate([carry] * (tile // LANES), axis=1)

            def add(i, _):
                at = pl.ds(pl.multiple_of(i * tile, LANES), tile)
                stage[s + r, :, at] = t_ref[j, :, at] + wide
                return 0

            lax.fori_loop(0, rows // tile - 1, add, 0, unroll=True)
            for i, sums in enumerate(parts):
                stage[s + r, :, pl.ds(rows - tile + i * LANES, LANES)] = sums
            pltpu.make_async_copy(stage.at[s + r], out_ref.at[j], sem).start()
    pltpu.make_async_copy(t_ref, out_ref, sem).wait()


def solution(mesh):
    n, groups = mesh.shape["dev"], mesh.shape["grp"]
    assert n >= 8 and not n & (n - 1)

    def local(amounts):
        chans, length = amounts.shape
        rows = length // n
        late = len(late_flips(n))
        relays = 2 * len(chips(n)[3])
        f32 = jnp.float32
        dma = pltpu.SemaphoreType.DMA
        regular = pltpu.SemaphoreType.REGULAR
        wide = (2 * LANES, 2 * LANES)
        table, run, weights = pl.pallas_call(
            functools.partial(exchange, n, groups),
            out_shape=[jax.ShapeDtypeStruct((n, chans, rows), f32),
                       jax.ShapeDtypeStruct((late, chans, LANES), f32),
                       jax.ShapeDtypeStruct(wide, jnp.bfloat16)],
            in_specs=[pl.BlockSpec(memory_space=pl.ANY)],
            out_specs=[pl.BlockSpec(memory_space=pltpu.VMEM)] * 3,
            scratch_shapes=[
                pltpu.VMEM((chans, length), f32),
                pltpu.VMEM((relays, chans, rows), f32),
                pltpu.VMEM((n, chans, LANES), f32),
                pltpu.VMEM((2, chans, LANES), f32),
                dma, dma, dma((1 + len(cuts_of(rows)),)), dma, dma((relays + 1,)),
                dma, dma, regular, regular, regular, regular, regular,
            ],
            compiler_params=pltpu.CompilerParams(
                collective_id=0, has_side_effects=True, vmem_limit_bytes=VMEM_GRANT),
            name="exchange",
        )(amounts)
        out = pl.pallas_call(
            functools.partial(write, n),
            out_shape=jax.ShapeDtypeStruct((n, chans, rows), f32),
            in_specs=[pl.BlockSpec(memory_space=pltpu.VMEM)] * 3,
            out_specs=pl.BlockSpec(memory_space=pl.ANY),
            scratch_shapes=[pltpu.VMEM((late, chans, rows), f32), dma],
            compiler_params=pltpu.CompilerParams(vmem_limit_bytes=VMEM_GRANT),
            name="write",
        )(table, run, weights)
        return out.reshape(n * chans, rows)

    return jax.shard_map(
        local,
        mesh=mesh,
        in_specs=(P("dev", "grp"),),
        out_specs=P(None, ("grp", "dev")),
        check_vma=False,
    )
```

```python
import functools

import jax
import jax.numpy as jnp
from jax import lax
from jax.experimental import pallas as pl
from jax.experimental.pallas import tpu as pltpu
from jax.sharding import PartitionSpec as P

MESH = pl.DeviceIdType.MESH
LANES = 128
VMEM_GRANT = 46 << 20


def flip(me, k):
    other, bit = me, 1
    while bit <= k:
        if k & bit:
            other = other + bit - 2 * bit * lax.rem(me // bit, 2)
        bit *= 2
    return other


def chips(n):
    across = (1 << (n.bit_length() - 2) // 2) - 1 << 1
    flips = range(2, n, 2)
    xs = [k for k in flips if not k & ~across]
    ys = [k for k in flips if not k & across]
    ds = [k for k in flips if k & across and k & ~across]
    return across, xs, ys, ds


def late_flips(n):
    _, xs, _, ds = chips(n)
    return [k + core for k in [*xs, *ds] for core in (0, 1)]


def tile_of(rows):
    return min(rows // 8, 2048)


def cuts_of(rows):
    cuts = [0, rows // 2, 3 * rows // 4, rows - tile_of(rows), rows]
    return list(zip(cuts[:-1], cuts[1:]))


def scan_tiles(blocks, w_ref, runs):
    chans, width = blocks[0].shape
    steps = width // LANES
    stack = jnp.concatenate(
        [block[:, j * LANES:(j + 1) * LANES] for block in blocks for j in range(steps)], axis=0)
    high = stack.astype(jnp.bfloat16)
    rest = stack - high.astype(jnp.float32)
    mid = rest.astype(jnp.bfloat16)
    low = (rest - mid.astype(jnp.float32)).astype(jnp.bfloat16)
    sums = jnp.dot(jnp.concatenate([high, mid], axis=1), w_ref[...], preferred_element_type=jnp.float32)
    sums = sums + jnp.dot(low, w_ref[:LANES, :], preferred_element_type=jnp.float32)
    outs, after = [], []
    for i, run in enumerate(runs):
        parts = []
        for j in range(i * steps, (i + 1) * steps):
            part = sums[j * chans:(j + 1) * chans]
            parts.append(part[:, :LANES] + run)
            run = run + part[:, LANES:]
        outs.append(parts)
        after.append(run)
    return outs, after


def last_lane(tile):
    return jnp.broadcast_to(tile[:, LANES - 1:], tile.shape)


def exchange(n, groups, x_ref, t_ref, run_ref, w_ref, x_vm, relay_vm, give_vm, carry_vm, group_vm,
             load_sem, send_sem, recv_sem, hsend_sem, hrecv_sem, csend_sem, crecv_sem, zsend_sem, zrecv_sem,
             note_sem, ready_sem, far_sem, hello_sem, zready_sem):
    me, grp = lax.axis_index("dev"), lax.axis_index("grp")
    core = lax.rem(me, 2)
    base = me - core
    partner = base + 1 - core
    chans, rows = t_ref.shape[1:]
    tile = tile_of(rows)
    pieces = cuts_of(rows)
    across, xs, ys, ds = chips(n)
    late = [flip(me, k) for k in late_flips(n)]

    def x_core(chip):
        return jnp.where((chip > across) & (lax.rem(chip // 2, across // 2 + 1) == 0), 0, 1)

    def y_core(chip):
        return jnp.where((chip <= across) & (chip > 0), 0, 1)

    def lead(chip):
        return jnp.where((chip == 0) & (grp == 0), 0, 1)

    def targets(k):
        chip = flip(base, k)
        return [chip + lead(chip), chip + 1 - lead(chip)]

    def signal(sem, **device):
        pl.semaphore_signal(sem, inc=1, device_id=device, device_id_type=MESH)

    barrier = pltpu.get_barrier_semaphore()

    @pl.when(core == lead(base))
    def _():
        for k in ys:
            signal(barrier, dev=flip(base, k) + y_core(flip(base, k)))
        for k in xs:
            signal(barrier, dev=flip(base, k) + x_core(flip(base, k)))

    @pl.when(core == 1)
    def _():
        signal(barrier, dev=base)

    @pl.when((me == 1) & (grp > 0))
    def _():
        signal(barrier, grp=grp - 1, dev=0)

    def at(j, lo=0, size=rows):
        return pl.ds(pl.multiple_of(j * rows + lo, LANES), size)

    load = pltpu.make_async_copy(x_ref, x_vm, load_sem)

    def remote(src, dst, sems, device):
        return pltpu.make_async_remote_copy(
            src_ref=src, dst_ref=dst, send_sem=sems[0], recv_sem=sems[1],
            device_id=device, device_id_type=MESH)

    def direct(j, sem, lo, hi, source=x_ref):
        remote(source.at[:, at(j, lo, hi - lo)], t_ref.at[me, :, pl.ds(lo, hi - lo)],
               (send_sem, recv_sem.at[sem]), {"dev": j}).start()

    def hop(j, slot, part, source):
        lo, hi = parts[part]
        remote(source.at[:, at(j, lo, hi - lo)], relay_vm.at[slot, :, pl.ds(lo, hi - lo)],
               (hsend_sem, hrecv_sem.at[slot, part]), {"dev": flip(me, ds[slot // 2] & across)}).start()

    def relay(j, slot, sem, lo, hi):
        source = flip(me, ds[slot // 2] & across)
        remote(relay_vm.at[slot, :, pl.ds(lo, hi - lo)], t_ref.at[source, :, pl.ds(lo, hi - lo)],
               (send_sem, recv_sem.at[sem]), {"dev": j}).start()

    x_blocks = [j for k in xs for j in targets(k)]
    y_blocks = [j for k in ys for j in targets(k)]
    d_blocks = [j for k in ds for j in targets(k)]

    half = rows // 2
    main = rows - tile
    parts = [(0, main), (main, rows)]
    x_side, y_side = core == x_core(base), core == y_core(base)

    after = jnp.where((me == 0) & (grp < groups - 1), 1, 0)
    faced = jnp.where(x_side, len(xs), 0) + jnp.where(y_side, len(ys), 0)
    pl.semaphore_wait(barrier, faced + 1 - core + after)

    @pl.when(x_side)
    def _():
        direct(x_blocks[0], 1, 0, half)

    @pl.when(y_side)
    def _():
        direct(y_blocks[0], 0, 0, main)

    load.start()

    @pl.when(core == 0)
    def _():
        signal(note_sem, dev=base + 1)

    pl.semaphore_wait(note_sem, 1)

    @pl.when((me == 1) & (grp < groups - 1))
    def _():
        signal(hello_sem, grp=grp + 1)

    @pl.when(core == 1)
    def _():
        signal(note_sem, dev=base)
        for k in [*xs, *ys]:
            signal(ready_sem, dev=targets(k)[0])

    pl.semaphore_wait(ready_sem, jnp.where(core == lead(base), len(xs) + len(ys), 1))

    @pl.when(core == lead(base))
    def _():
        signal(ready_sem, dev=partner)

    @pl.when(core == 1)
    def _():
        for k in xs:
            for j in targets(k):
                signal(far_sem, dev=j)

    for slot, j in enumerate(d_blocks):
        hop(j, slot, 0, x_ref)

    @pl.when(jnp.logical_not(y_side))
    def _():
        direct(y_blocks[0], 0, 0, main)

    for j in y_blocks[1:]:
        direct(j, 0, 0, main)
    direct(partner, 0, 0, rows)
    load.wait()

    shape = (2 * LANES, 2 * LANES)
    row = lax.rem(lax.broadcasted_iota(jnp.int32, shape, 0), LANES)
    col = lax.broadcasted_iota(jnp.int32, shape, 1)
    w_ref[...] = jnp.where((row < col) | (col >= LANES), 1.0, 0.0).astype(jnp.bfloat16)

    def range_total(j, total):
        give_vm[j] = total

        def one(i, acc):
            block = x_vm[:, at(j, i * tile, tile)]
            parts = [block[:, s * LANES:(s + 1) * LANES] for s in range(tile // LANES)]
            while len(parts) > 1:
                parts = [a + b for a, b in zip(parts[::2], parts[1::2])] + parts[len(parts) & ~1:]
            return acc + parts[0]

        acc = lax.fori_loop(0, rows // tile, one, jnp.zeros((chans, LANES), jnp.float32))
        return total + jnp.broadcast_to(jnp.sum(acc, axis=1, keepdims=True), acc.shape)

    total = lax.fori_loop(0, n, range_total, jnp.zeros((chans, LANES), jnp.float32))

    pl.semaphore_wait(far_sem, len(xs))

    @pl.when((me == 1) & (grp > 0))
    def _():
        pl.semaphore_wait(hello_sem, 1)
        signal(zready_sem, grp=grp - 1)

    @pl.when(grp < groups - 1)
    def _():
        pl.semaphore_wait(zready_sem, 1)

    @pl.when((me == 1) & (grp < groups - 1))
    def _():
        for k in range(1, n):
            signal(zready_sem, dev=flip(me, k))

    def pass_on():
        return remote(group_vm.at[1], group_vm.at[0], (zsend_sem, zrecv_sem), {"grp": grp + 1})

    @pl.when(grp == 0)
    def _():
        group_vm[0] = jnp.zeros_like(total)

    @pl.when(grp > 0)
    def _():
        pass_on().wait_recv()

    before = group_vm[0]
    group_vm[1] = before + total
    for j in range(n):
        give_vm[j] = give_vm[j] + before
    carry_vm[me] = give_vm[me]

    @pl.when(grp < groups - 1)
    def _():
        pass_on().start()

    lane = lax.broadcasted_iota(jnp.int32, (chans, LANES), 1)
    for j in range(n):
        end = pl.ds((j + 1) * rows - LANES, LANES)
        x_vm[:, end] = jnp.where(lane == LANES - 1, give_vm[j], x_vm[:, end])
    given = remote(give_vm.at[partner], carry_vm.at[me], (csend_sem, crecv_sem), {"dev": partner})
    given.start()
    for slot, j in enumerate(d_blocks):
        hop(j, slot, 1, x_vm)
    for j in y_blocks:
        direct(j, 0, main, rows, x_vm)

    @pl.when(jnp.logical_not(x_side))
    def _():
        direct(x_blocks[0], 1, 0, half)

    for slot, j in enumerate(x_blocks):
        for i, (lo, hi) in enumerate(pieces):
            if slot or i:
                direct(j, 1 + i, lo, hi, x_vm if hi == rows else x_ref)

    def scan(blocks, lo, hi, runs):
        width = min(hi - lo, 4 * tile // len(blocks))

        def one(i, runs):
            start = lo + i * width
            tiles = [source[:, pl.ds(pl.multiple_of(offset + start, LANES), width)] for source, offset, _ in blocks]
            outs, runs = scan_tiles(tiles, w_ref, runs)
            for (_, _, dest), parts in zip(blocks, outs):
                for j, sums in enumerate(parts):
                    dest[:, pl.ds(pl.multiple_of(start + j * LANES, LANES), LANES)] = sums
            return tuple(runs)

        return lax.fori_loop(0, (hi - lo) // width, one, tuple(runs))

    def in_place(j):
        return t_ref.at[j], 0, t_ref.at[j]

    def arrived(sem, blocks, lo=0, hi=rows):
        span = t_ref.at[pl.ds(0, blocks), :, pl.ds(lo, hi - lo)]
        remote(span, span, (send_sem, recv_sem.at[sem]), {"dev": partner}).wait_recv()

    scan([(x_vm, me * rows, t_ref.at[me])], 0, rows, [carry_vm[me]])
    def forward(slot, part):
        lo, hi = parts[part]
        span = relay_vm.at[slot, :, pl.ds(lo, hi - lo)]
        remote(span, span, (hsend_sem, hrecv_sem.at[slot, part]), {"dev": partner}).wait_recv()
        j = targets(ds[slot // 2] & ~across)[slot % 2]
        for i, (start, end) in enumerate(pieces):
            if lo <= start < hi:
                relay(j, slot, 1 + i, start, end)

    for slot in range(len(d_blocks)):
        forward(slot, 0)
    for slot in range(len(d_blocks)):
        forward(slot, 1)

    given.wait()
    arrived(0, 1 + len(y_blocks))
    scan([in_place(partner)], 0, rows, [carry_vm[partner]])
    for s in range(0, len(y_blocks), 2):
        pair = y_blocks[s:s + 2]
        runs = [last_lane(t_ref[j, :, pl.ds(rows - LANES, LANES)]) for j in pair]
        scan([in_place(j) for j in pair], 0, rows, runs)

    for i in range(len(late)):
        run_ref[i] = jnp.zeros((chans, LANES), jnp.float32)
    for i, (lo, hi) in enumerate(pieces[:-1]):
        arrived(1 + i, len(late), lo, hi)
        for s in range(0, len(late), 4):
            four = late[s:s + 4]
            runs = scan([in_place(j) for j in four], lo, hi, [run_ref[s + r] for r in range(len(four))])
            for r, run in enumerate(runs):
                run_ref[s + r] = run

    @pl.when(grp < groups - 1)
    def _():
        pass_on().wait_send()

    remote(relay_vm, relay_vm, (hsend_sem, hrecv_sem.at[0, 0]), {"dev": partner}).wait_send()
    sent = x_vm.at[:, pl.ds(0, (n - 1) * rows)]
    remote(sent, sent, (send_sem, recv_sem.at[0]), {"dev": partner}).wait_send()
    arrived(len(pieces), len(late), *pieces[-1])


def write(n, t_ref, run_ref, w_ref, out_ref, stage, sem):
    me = lax.axis_index("dev")
    rows = t_ref.shape[2]
    tile = tile_of(rows)
    late = late_flips(n)
    last = pl.ds(rows - tile, tile)

    for k in range(n):
        if k not in late:
            j = flip(me, k)
            pltpu.make_async_copy(t_ref.at[j], out_ref.at[j], sem).start()
    for s in range(0, len(late), 4):
        four = [flip(me, k) for k in late[s:s + 4]]
        carries = [last_lane(t_ref[j, :, pl.ds(rows - LANES, LANES)]) for j in four]
        runs = [run_ref[s + r] + carry for r, carry in enumerate(carries)]
        outs, _ = scan_tiles([t_ref[j, :, last] for j in four], w_ref, runs)
        for r, (j, carry, parts) in enumerate(zip(four, carries, outs)):
            wide = jnp.concatenate([carry] * (tile // LANES), axis=1)

            def add(i, _):
                at = pl.ds(pl.multiple_of(i * tile, LANES), tile)
                stage[s + r, :, at] = t_ref[j, :, at] + wide
                return 0

            lax.fori_loop(0, rows // tile - 1, add, 0, unroll=True)
            for i, sums in enumerate(parts):
                stage[s + r, :, pl.ds(rows - tile + i * LANES, LANES)] = sums
            pltpu.make_async_copy(stage.at[s + r], out_ref.at[j], sem).start()
    pltpu.make_async_copy(t_ref, out_ref, sem).wait()


def solution(mesh):
    n, groups = mesh.shape["dev"], mesh.shape["grp"]
    assert n >= 8 and not n & (n - 1)

    def local(amounts):
        chans, length = amounts.shape
        rows = length // n
        late = len(late_flips(n))
        relays = 2 * len(chips(n)[3])
        f32 = jnp.float32
        dma = pltpu.SemaphoreType.DMA
        regular = pltpu.SemaphoreType.REGULAR
        wide = (2 * LANES, 2 * LANES)
        table, run, weights = pl.pallas_call(
            functools.partial(exchange, n, groups),
            out_shape=[jax.ShapeDtypeStruct((n, chans, rows), f32),
                       jax.ShapeDtypeStruct((late, chans, LANES), f32),
                       jax.ShapeDtypeStruct(wide, jnp.bfloat16)],
            in_specs=[pl.BlockSpec(memory_space=pl.ANY)],
            out_specs=[pl.BlockSpec(memory_space=pltpu.VMEM)] * 3,
            scratch_shapes=[
                pltpu.VMEM((chans, length), f32),
                pltpu.VMEM((relays, chans, rows), f32),
                pltpu.VMEM((n, chans, LANES), f32),
                pltpu.VMEM((n, chans, LANES), f32),
                pltpu.VMEM((2, chans, LANES), f32),
                dma, dma, dma((1 + len(cuts_of(rows)),)), dma, dma((relays, 2)),
                dma, dma, dma, dma, regular, regular, regular, regular, regular,
            ],
            compiler_params=pltpu.CompilerParams(
                collective_id=0, has_side_effects=True, vmem_limit_bytes=VMEM_GRANT),
            name="exchange",
        )(amounts)
        out = pl.pallas_call(
            functools.partial(write, n),
            out_shape=jax.ShapeDtypeStruct((n, chans, rows), f32),
            in_specs=[pl.BlockSpec(memory_space=pltpu.VMEM)] * 3,
            out_specs=pl.BlockSpec(memory_space=pl.ANY),
            scratch_shapes=[pltpu.VMEM((late, chans, rows), f32), dma],
            compiler_params=pltpu.CompilerParams(vmem_limit_bytes=VMEM_GRANT),
            name="write",
        )(table, run, weights)
        return out.reshape(n * chans, rows)

    return jax.shard_map(
        local,
        mesh=mesh,
        in_specs=(P("dev", "grp"),),
        out_specs=P(None, ("grp", "dev")),
        check_vma=False,
    )
```

```python
import functools

import jax
import jax.numpy as jnp
from jax import lax
from jax.experimental import pallas as pl
from jax.experimental.pallas import tpu as pltpu
from jax.sharding import PartitionSpec as P

MESH = pl.DeviceIdType.MESH
LANES = 128
VMEM_GRANT = 46 << 20


def flip(me, k):
    other, bit = me, 1
    while bit <= k:
        if k & bit:
            other = other + bit - 2 * bit * lax.rem(me // bit, 2)
        bit *= 2
    return other


def chips(n):
    across = (1 << (n.bit_length() - 2) // 2) - 1 << 1
    flips = range(2, n, 2)
    xs = [k for k in flips if not k & ~across]
    ys = [k for k in flips if not k & across]
    ds = [k for k in flips if k & across and k & ~across]
    return across, xs, ys, ds


def late_flips(n):
    _, xs, _, ds = chips(n)
    return [k + core for k in [*xs, *ds] for core in (0, 1)]


def tile_of(rows):
    return min(rows // 8, 2048)


def cuts_of(rows):
    cuts = [0, rows // 2, 3 * rows // 4, rows - tile_of(rows), rows]
    return list(zip(cuts[:-1], cuts[1:]))


def scan_tiles(blocks, w_ref, runs):
    chans, width = blocks[0].shape
    steps = width // LANES
    stack = jnp.concatenate(
        [block[:, j * LANES:(j + 1) * LANES] for block in blocks for j in range(steps)], axis=0)
    high = stack.astype(jnp.bfloat16)
    rest = stack - high.astype(jnp.float32)
    mid = rest.astype(jnp.bfloat16)
    low = (rest - mid.astype(jnp.float32)).astype(jnp.bfloat16)
    sums = jnp.dot(jnp.concatenate([high, mid], axis=1), w_ref[...], preferred_element_type=jnp.float32)
    sums = sums + jnp.dot(low, w_ref[:LANES, :], preferred_element_type=jnp.float32)
    outs, after = [], []
    for i, run in enumerate(runs):
        parts = []
        for j in range(i * steps, (i + 1) * steps):
            part = sums[j * chans:(j + 1) * chans]
            parts.append(part[:, :LANES] + run)
            run = run + part[:, LANES:]
        outs.append(parts)
        after.append(run)
    return outs, after


def last_lane(tile):
    return jnp.broadcast_to(tile[:, LANES - 1:], tile.shape)


def exchange(n, groups, x_ref, t_ref, run_ref, w_ref, x_vm, relay_vm, give_vm, group_vm,
             load_sem, send_sem, recv_sem, hsend_sem, hrecv_sem, zsend_sem, zrecv_sem,
             note_sem, ready_sem, far_sem, hello_sem, zready_sem):
    me, grp = lax.axis_index("dev"), lax.axis_index("grp")
    core = lax.rem(me, 2)
    base = me - core
    partner = base + 1 - core
    chans, rows = t_ref.shape[1:]
    tile = tile_of(rows)
    pieces = cuts_of(rows)
    across, xs, ys, ds = chips(n)
    late = [flip(me, k) for k in late_flips(n)]

    def x_core(chip):
        return jnp.where((chip > across) & (lax.rem(chip // 2, across // 2 + 1) == 0), 0, 1)

    def y_core(chip):
        return jnp.where((chip <= across) & (chip > 0), 0, 1)

    def lead(chip):
        return jnp.where((chip == 0) & (grp == 0), 0, 1)

    def targets(k):
        chip = flip(base, k)
        return [chip + lead(chip), chip + 1 - lead(chip)]

    def signal(sem, **device):
        pl.semaphore_signal(sem, inc=1, device_id=device, device_id_type=MESH)

    barrier = pltpu.get_barrier_semaphore()

    @pl.when(core == lead(base))
    def _():
        for k in ys:
            signal(barrier, dev=flip(base, k) + y_core(flip(base, k)))
        for k in xs:
            signal(barrier, dev=flip(base, k) + x_core(flip(base, k)))

    @pl.when(core == 1)
    def _():
        signal(barrier, dev=base)

    @pl.when((me == 1) & (grp > 0))
    def _():
        signal(barrier, grp=grp - 1, dev=0)

    def at(j, lo=0, size=rows):
        return pl.ds(pl.multiple_of(j * rows + lo, LANES), size)

    load = pltpu.make_async_copy(x_ref, x_vm, load_sem)

    def remote(src, dst, sems, device):
        return pltpu.make_async_remote_copy(
            src_ref=src, dst_ref=dst, send_sem=sems[0], recv_sem=sems[1],
            device_id=device, device_id_type=MESH)

    def direct(j, sem, lo, hi, source=x_ref):
        remote(source.at[:, at(j, lo, hi - lo)], t_ref.at[me, :, pl.ds(lo, hi - lo)],
               (send_sem, recv_sem.at[sem]), {"dev": j}).start()

    def hop(j, slot, part, source):
        lo, hi = parts[part]
        remote(source.at[:, at(j, lo, hi - lo)], relay_vm.at[slot, :, pl.ds(lo, hi - lo)],
               (hsend_sem, hrecv_sem.at[len(d_blocks) if part else slot]), {"dev": flip(me, ds[slot // 2] & across)}).start()

    def relay(j, slot, sem, lo, hi):
        source = flip(me, ds[slot // 2] & across)
        remote(relay_vm.at[slot, :, pl.ds(lo, hi - lo)], t_ref.at[source, :, pl.ds(lo, hi - lo)],
               (send_sem, recv_sem.at[sem]), {"dev": j}).start()

    x_blocks = [j for k in xs for j in targets(k)]
    y_blocks = [j for k in ys for j in targets(k)]
    d_blocks = [j for k in ds for j in targets(k)]

    half = rows // 2
    main = rows - tile
    parts = [(0, main), (main, rows)]
    x_side, y_side = core == x_core(base), core == y_core(base)

    after = jnp.where((me == 0) & (grp < groups - 1), 1, 0)
    faced = jnp.where(x_side, len(xs), 0) + jnp.where(y_side, len(ys), 0)
    pl.semaphore_wait(barrier, faced + 1 - core + after)

    @pl.when(x_side)
    def _():
        direct(x_blocks[0], 1, 0, half)

    @pl.when(y_side)
    def _():
        direct(y_blocks[0], 0, 0, main)

    load.start()

    @pl.when(core == 0)
    def _():
        signal(note_sem, dev=base + 1)

    pl.semaphore_wait(note_sem, 1)

    @pl.when((me == 1) & (grp < groups - 1))
    def _():
        signal(hello_sem, grp=grp + 1)

    @pl.when(core == 1)
    def _():
        signal(note_sem, dev=base)
        for k in [*xs, *ys]:
            signal(ready_sem, dev=targets(k)[0])

    pl.semaphore_wait(ready_sem, jnp.where(core == lead(base), len(xs) + len(ys), 1))

    @pl.when(core == lead(base))
    def _():
        signal(ready_sem, dev=partner)

    @pl.when(core == 1)
    def _():
        for k in xs:
            for j in targets(k):
                signal(far_sem, dev=j)

    for slot, j in enumerate(d_blocks):
        hop(j, slot, 0, x_ref)

    @pl.when(jnp.logical_not(y_side))
    def _():
        direct(y_blocks[0], 0, 0, main)

    for j in y_blocks[1:]:
        direct(j, 0, 0, main)
    direct(partner, 0, 0, main)
    load.wait()

    shape = (2 * LANES, 2 * LANES)
    row = lax.rem(lax.broadcasted_iota(jnp.int32, shape, 0), LANES)
    col = lax.broadcasted_iota(jnp.int32, shape, 1)
    w_ref[...] = jnp.where((row < col) | (col >= LANES), 1.0, 0.0).astype(jnp.bfloat16)

    def range_total(j, total):
        give_vm[j] = total

        def one(i, acc):
            block = x_vm[:, at(j, i * tile, tile)]
            parts = [block[:, s * LANES:(s + 1) * LANES] for s in range(tile // LANES)]
            while len(parts) > 1:
                parts = [a + b for a, b in zip(parts[::2], parts[1::2])] + parts[len(parts) & ~1:]
            return acc + parts[0]

        acc = lax.fori_loop(0, rows // tile, one, jnp.zeros((chans, LANES), jnp.float32))
        return total + jnp.broadcast_to(jnp.sum(acc, axis=1, keepdims=True), acc.shape)

    total = lax.fori_loop(0, n, range_total, jnp.zeros((chans, LANES), jnp.float32))

    pl.semaphore_wait(far_sem, len(xs))

    @pl.when((me == 1) & (grp > 0))
    def _():
        pl.semaphore_wait(hello_sem, 1)
        signal(zready_sem, grp=grp - 1)

    @pl.when(grp < groups - 1)
    def _():
        pl.semaphore_wait(zready_sem, 1)

    @pl.when((me == 1) & (grp < groups - 1))
    def _():
        for k in range(1, n):
            signal(zready_sem, dev=flip(me, k))

    def pass_on():
        return remote(group_vm.at[1], group_vm.at[0], (zsend_sem, zrecv_sem), {"grp": grp + 1})

    @pl.when(grp == 0)
    def _():
        group_vm[0] = jnp.zeros_like(total)

    @pl.when(grp > 0)
    def _():
        pass_on().wait_recv()

    before = group_vm[0]
    group_vm[1] = before + total
    for j in range(n):
        give_vm[j] = give_vm[j] + before

    @pl.when(grp < groups - 1)
    def _():
        pass_on().start()

    lane = lax.broadcasted_iota(jnp.int32, (chans, LANES), 1)
    for j in range(n):
        end = pl.ds((j + 1) * rows - LANES, LANES)
        x_vm[:, end] = jnp.where(lane == LANES - 1, give_vm[j], x_vm[:, end])
    direct(partner, 0, main, rows, x_vm)
    for slot, j in enumerate(d_blocks):
        hop(j, slot, 1, x_vm)
    for j in y_blocks:
        direct(j, 0, main, rows, x_vm)

    @pl.when(jnp.logical_not(x_side))
    def _():
        direct(x_blocks[0], 1, 0, half)

    for slot, j in enumerate(x_blocks):
        for i, (lo, hi) in enumerate(pieces):
            if slot or i:
                direct(j, 1 + i, lo, hi, x_vm if hi == rows else x_ref)

    def scan(blocks, lo, hi, runs):
        width = min(hi - lo, 4 * tile // len(blocks))

        def one(i, runs):
            start = lo + i * width
            tiles = [source[:, pl.ds(pl.multiple_of(offset + start, LANES), width)] for source, offset, _ in blocks]
            outs, runs = scan_tiles(tiles, w_ref, runs)
            for (_, _, dest), parts in zip(blocks, outs):
                for j, sums in enumerate(parts):
                    dest[:, pl.ds(pl.multiple_of(start + j * LANES, LANES), LANES)] = sums
            return tuple(runs)

        return lax.fori_loop(0, (hi - lo) // width, one, tuple(runs))

    def in_place(j):
        return t_ref.at[j], 0, t_ref.at[j]

    def arrived(sem, blocks, lo=0, hi=rows):
        span = t_ref.at[pl.ds(0, blocks), :, pl.ds(lo, hi - lo)]
        remote(span, span, (send_sem, recv_sem.at[sem]), {"dev": partner}).wait_recv()

    scan([(x_vm, me * rows, t_ref.at[me])], 0, rows, [give_vm[me]])
    def forward(slots, part):
        lo, hi = parts[part]
        span = relay_vm.at[pl.ds(slots[0], len(slots)), :, pl.ds(lo, hi - lo)]
        sem = hrecv_sem.at[len(d_blocks) if part else slots[0]]
        remote(span, span, (hsend_sem, sem), {"dev": partner}).wait_recv()
        for slot in slots:
            j = targets(ds[slot // 2] & ~across)[slot % 2]
            for i, (start, end) in enumerate(pieces):
                if lo <= start < hi:
                    relay(j, slot, 1 + i, start, end)

    for slot in range(len(d_blocks)):
        forward([slot], 0)
    forward(range(len(d_blocks)), 1)

    arrived(0, 1 + len(y_blocks))
    scan([in_place(partner)], 0, rows, [last_lane(t_ref[partner, :, pl.ds(rows - LANES, LANES)])])
    for s in range(0, len(y_blocks), 2):
        pair = y_blocks[s:s + 2]
        runs = [last_lane(t_ref[j, :, pl.ds(rows - LANES, LANES)]) for j in pair]
        scan([in_place(j) for j in pair], 0, rows, runs)

    for i in range(len(late)):
        run_ref[i] = jnp.zeros((chans, LANES), jnp.float32)
    for i, (lo, hi) in enumerate(pieces[:-1]):
        arrived(1 + i, len(late), lo, hi)
        for s in range(0, len(late), 4):
            four = late[s:s + 4]
            runs = scan([in_place(j) for j in four], lo, hi, [run_ref[s + r] for r in range(len(four))])
            for r, run in enumerate(runs):
                run_ref[s + r] = run

    @pl.when(grp < groups - 1)
    def _():
        pass_on().wait_send()

    remote(relay_vm, relay_vm, (hsend_sem, hrecv_sem.at[0]), {"dev": partner}).wait_send()
    sent = x_vm.at[:, pl.ds(0, (n - 1) * rows)]
    remote(sent, sent, (send_sem, recv_sem.at[0]), {"dev": partner}).wait_send()
    arrived(len(pieces), len(late), *pieces[-1])


def write(n, t_ref, run_ref, w_ref, out_ref, stage, sem):
    me = lax.axis_index("dev")
    rows = t_ref.shape[2]
    tile = tile_of(rows)
    late = late_flips(n)
    last = pl.ds(rows - tile, tile)

    for k in range(n):
        if k not in late:
            j = flip(me, k)
            pltpu.make_async_copy(t_ref.at[j], out_ref.at[j], sem).start()
    for s in range(0, len(late), 4):
        four = [flip(me, k) for k in late[s:s + 4]]
        carries = [last_lane(t_ref[j, :, pl.ds(rows - LANES, LANES)]) for j in four]
        runs = [run_ref[s + r] + carry for r, carry in enumerate(carries)]
        outs, _ = scan_tiles([t_ref[j, :, last] for j in four], w_ref, runs)
        for r, (j, carry, parts) in enumerate(zip(four, carries, outs)):
            wide = jnp.concatenate([carry] * (tile // LANES), axis=1)

            def add(i, _):
                at = pl.ds(pl.multiple_of(i * tile, LANES), tile)
                stage[s + r, :, at] = t_ref[j, :, at] + wide
                return 0

            lax.fori_loop(0, rows // tile - 1, add, 0, unroll=True)
            for i, sums in enumerate(parts):
                stage[s + r, :, pl.ds(rows - tile + i * LANES, LANES)] = sums
            pltpu.make_async_copy(stage.at[s + r], out_ref.at[j], sem).start()
    pltpu.make_async_copy(t_ref, out_ref, sem).wait()


def solution(mesh):
    n, groups = mesh.shape["dev"], mesh.shape["grp"]
    assert n >= 8 and not n & (n - 1)

    def local(amounts):
        chans, length = amounts.shape
        rows = length // n
        late = len(late_flips(n))
        relays = 2 * len(chips(n)[3])
        f32 = jnp.float32
        dma = pltpu.SemaphoreType.DMA
        regular = pltpu.SemaphoreType.REGULAR
        wide = (2 * LANES, 2 * LANES)
        table, run, weights = pl.pallas_call(
            functools.partial(exchange, n, groups),
            out_shape=[jax.ShapeDtypeStruct((n, chans, rows), f32),
                       jax.ShapeDtypeStruct((late, chans, LANES), f32),
                       jax.ShapeDtypeStruct(wide, jnp.bfloat16)],
            in_specs=[pl.BlockSpec(memory_space=pl.ANY)],
            out_specs=[pl.BlockSpec(memory_space=pltpu.VMEM)] * 3,
            scratch_shapes=[
                pltpu.VMEM((chans, length), f32),
                pltpu.VMEM((relays, chans, rows), f32),
                pltpu.VMEM((n, chans, LANES), f32),
                pltpu.VMEM((2, chans, LANES), f32),
                dma, dma, dma((1 + len(cuts_of(rows)),)), dma, dma((relays + 1,)),
                dma, dma, regular, regular, regular, regular, regular,
            ],
            compiler_params=pltpu.CompilerParams(
                collective_id=0, has_side_effects=True, vmem_limit_bytes=VMEM_GRANT),
            name="exchange",
        )(amounts)
        out = pl.pallas_call(
            functools.partial(write, n),
            out_shape=jax.ShapeDtypeStruct((n, chans, rows), f32),
            in_specs=[pl.BlockSpec(memory_space=pltpu.VMEM)] * 3,
            out_specs=pl.BlockSpec(memory_space=pl.ANY),
            scratch_shapes=[pltpu.VMEM((late, chans, rows), f32), dma],
            compiler_params=pltpu.CompilerParams(vmem_limit_bytes=VMEM_GRANT),
            name="write",
        )(table, run, weights)
        return out.reshape(n * chans, rows)

    return jax.shard_map(
        local,
        mesh=mesh,
        in_specs=(P("dev", "grp"),),
        out_specs=P(None, ("grp", "dev")),
        check_vma=False,
    )
```
